256 devices in a mesh: grp: 32 (over z, x), mem: 8 (over y, core).
Axes of the slice: x: 4, y: 4, z: 8, core: 2. Of those that a mesh axis runs over, the one named last changes fastest.
Arguments:
- right_side: float32 [32, 524288], P(None, ('grp', 'mem')), may hold values from -6 to 6
- fine_tiles: float32 [4096, 3, 128, 128], P(('grp', 'mem')), may hold values from -0.13492627 to 6.130239
- fine_columns: int32 [4096, 3], P(('grp', 'mem')), may hold values from 0 to 19, as said below
- fine_sends: int32 [512, 256], P(('grp', 'mem')), may hold values from 0 to 2047, as said below
- fine_weights: float32 [524288], P(('grp', 'mem')), may hold values from 0.5 to 2
- fine_groups: int32 [524288], P(('grp', 'mem')), may hold values from 0 to 255, as said below
- group_tiles: float32 [512, 3, 128, 128], P('grp'), may hold values from -1.0794102 to 49.0419102
- group_columns: int32 [512, 3], P('grp'), may hold values from 0 to 17, as said below
- group_sends: int32 [64, 128], P('grp'), may hold values from 0 to 2047, as said below
- group_weights: float32 [65536], P('grp'), may hold values from 0.5 to 2
- group_groups: int32 [65536], P('grp'), may hold values from 0 to 63, as said below
- coarse_tiles: float32 [16, 3, 128, 128], replicated, may hold values from -2.1588203 to 98.08382034355964
- coarse_columns: int32 [16, 3], replicated, may hold values from 0 to 15, as said below
Outputs:
- solution: float32 [32, 524288], P(None, ('grp', 'mem'))
- residual: float32 [32, 524288], P(None, ('grp', 'mem'))
The draws below stay inside these ranges and needn't reach their ends.
Inputs may be any that keep to these rules, and one draw needn't show every extreme that they name: `fine_columns`: fine tiles: within each owner's 16 tile rows, entry 0 is the tile row's own index; entries 1 each name a distinct block of the extended vector (16 own blocks, then 2 from the lower neighbour, then 2 from the higher), and so do entries 2; every halo block is named by entries 2. `fine_sends`: each list holds 256 distinct rows of its owner; list 2 o goes to owner o - 1, list 2 o + 1 to owner o + 1. `fine_groups`: each aggregate of an owner takes exactly 8 of its rows. `group_columns`: as for fine_columns, per group, with 16 tile rows and 2 halo blocks. `group_sends`: each list holds 128 distinct rows of its group. `group_groups`: each aggregate of a group takes exactly 32 of its rows. `coarse_columns`: entry 0 is the tile row's own index; entries 1 name each block once, and so do entries 2.
All inputs are finite; a program needn't handle non-finite values.
Results may differ from the reference program's by a relative error of at most 0.0003.
Values sent between devices are 32-bit elements; how exact they have to be, the bound alone decides.
No kernel may reach another device: no remote copies, remote signals or barrier semaphores. Data moves between devices by JAX's collectives and lax.ppermute only.
A program may use at most 128 MiB of HBM per device.

```python
import functools
import math
import jax
import jax.numpy as jnp
from jax import lax

NRHS = 32
R0 = 2048
TILE = 128
HALO0 = 256
HALO1 = 128
AGG1 = 8
AGG2 = 32
ITERS = 2
NB0 = 16
HB0 = 4
ROWS1 = 2048
NB1 = 16
HB1 = 2
ROWS2 = 64
COARSE = 2048
NB2 = 16
UNKNOWNS = 524288
N_GRP = 32
N_MEM = 8


PULL = 0.15


ROUGH = 0.25


def tile_block(key, block_count, scale):
    entry_key, boost_key = jax.random.split(key)
    reach = 3 * TILE
    entries = jax.random.uniform(entry_key, (block_count, 3, TILE, TILE), jnp.float32, -1.0, 1.0)
    entries = ROUGH * (3.0 / reach) ** 0.5 * entries - PULL / reach
    boost = jax.random.uniform(boost_key, (block_count, TILE), jnp.float32, 3.0, 6.0)
    entries = boost[:, None, :, None] * entries
    identity = jnp.eye(TILE, dtype=jnp.float32)
    entries = entries.at[:, 0].add(boost[:, :, None] * identity[None])
    return scale * entries


def column_block(key, block_count, halo_blocks):
    first_key, second_key, place_key = jax.random.split(key, 3)
    own_index = jnp.arange(block_count, dtype=jnp.int32)
    first_col = jax.random.permutation(first_key, block_count + halo_blocks)[:block_count].astype(jnp.int32)
    second_col = jax.random.permutation(second_key, block_count).astype(jnp.int32)
    if halo_blocks > 0:
        positions = jax.random.permutation(place_key, block_count)[:halo_blocks]
        second_col = second_col.at[positions].set(block_count + jnp.arange(halo_blocks, dtype=jnp.int32))
    return jnp.stack([own_index, first_col, second_col], axis=1)


def send_block(key, row_count, list_length):
    return jax.random.permutation(key, row_count)[:list_length].astype(jnp.int32)


def group_block(key, row_count, group_size):
    return (jax.random.permutation(key, row_count) // group_size).astype(jnp.int32)


def draw_right_side(key, part):
    normal_part = jax.random.normal(jax.random.fold_in(key, 11), (NRHS, R0 * N_GRP * N_MEM), jnp.float32)
    return jnp.clip(normal_part, -6.0, 6.0)


def draw_fine_tiles(key, part):
    return tile_block(jax.random.fold_in(key, 21), NB0 * N_GRP * N_MEM, 1.0)


def draw_group_tiles(key, part):
    return tile_block(jax.random.fold_in(key, 22), NB1 * N_GRP, 1.0 * AGG1)


def draw_coarse_tiles(key, part):
    return tile_block(jax.random.fold_in(key, 23), NB2, (1.0 * AGG1 * AGG2) ** 0.5)


def draw_fine_columns(key, part):
    key_list = jax.random.split(jax.random.fold_in(key, 31), N_GRP * N_MEM)
    return jax.vmap(lambda subkey: column_block(subkey, NB0, HB0))(key_list).reshape(-1, 3)


def draw_group_columns(key, part):
    key_list = jax.random.split(jax.random.fold_in(key, 32), N_GRP)
    return jax.vmap(lambda subkey: column_block(subkey, NB1, HB1))(key_list).reshape(-1, 3)


def draw_coarse_columns(key, part):
    return column_block(jax.random.fold_in(key, 33), NB2, 0)


def draw_fine_sends(key, part):
    key_list = jax.random.split(jax.random.fold_in(key, 41), 2 * N_GRP * N_MEM)
    return jax.vmap(lambda subkey: send_block(subkey, R0, HALO0))(key_list)


def draw_group_sends(key, part):
    key_list = jax.random.split(jax.random.fold_in(key, 42), 2 * N_GRP)
    return jax.vmap(lambda subkey: send_block(subkey, ROWS1, HALO1))(key_list)


def draw_fine_groups(key, part):
    key_list = jax.random.split(jax.random.fold_in(key, 51), N_GRP * N_MEM)
    return jax.vmap(lambda subkey: group_block(subkey, R0, AGG1))(key_list).reshape(-1)


def draw_group_groups(key, part):
    key_list = jax.random.split(jax.random.fold_in(key, 52), N_GRP)
    return jax.vmap(lambda subkey: group_block(subkey, ROWS1, AGG2))(key_list).reshape(-1)


def shard_levels(key, extent, cuts, least, largest):
    def one(position, shards_of):
        draws = jax.random.uniform(jax.random.fold_in(jax.random.fold_in(key, 6), position), (shards_of,), jnp.float32, least / len(cuts), largest / len(cuts))
        return jnp.repeat(jnp.exp(draws), extent[position] // shards_of).reshape((-1,) + (1,) * (len(extent) - position - 1))

    level = one(*cuts[0])
    for cut in cuts[1:]:
        level = level * one(*cut)
    return level


def setup_inputs(seed: int = 0) -> dict:
    keys = jax.random.split(jax.random.key(seed), 14)
    return {
        "right_side": draw_right_side(jax.random.fold_in(keys[13], 71), 0),
        "fine_tiles": draw_fine_tiles(jax.random.fold_in(keys[13], 71), 0),
        "fine_columns": draw_fine_columns(jax.random.fold_in(keys[13], 71), 0),
        "fine_sends": draw_fine_sends(jax.random.fold_in(keys[13], 71), 0),
        "fine_weights": jnp.clip(jnp.exp(math.log(2.0) - 1.3862944 * jax.random.uniform(keys[4], (UNKNOWNS,), jnp.float32) ** shard_levels(keys[4], (UNKNOWNS,), ((0, 256),), -0.2, 0.2)), 0.5, 2.0),
        "fine_groups": draw_fine_groups(jax.random.fold_in(keys[13], 71), 0),
        "group_tiles": draw_group_tiles(jax.random.fold_in(keys[13], 71), 0),
        "group_columns": draw_group_columns(jax.random.fold_in(keys[13], 71), 0),
        "group_sends": draw_group_sends(jax.random.fold_in(keys[13], 71), 0),
        "group_weights": jnp.clip(jnp.exp(math.log(2.0) - 1.3862944 * jax.random.uniform(keys[9], (ROWS1 * N_GRP,), jnp.float32) ** shard_levels(keys[9], (ROWS1 * N_GRP,), ((0, 32),), -0.2, 0.2)), 0.5, 2.0),
        "group_groups": draw_group_groups(jax.random.fold_in(keys[13], 71), 0),
        "coarse_tiles": draw_coarse_tiles(jax.random.fold_in(keys[13], 71), 0),
        "coarse_columns": draw_coarse_columns(jax.random.fold_in(keys[13], 71), 0),
    }


RELAXATION = 0.7


def tile_apply(tile_set, tile_cols, extended):
    tile_width = tile_set.shape[2]
    blocks = extended.reshape(extended.shape[0], -1, tile_width)
    picked = blocks[:, tile_cols, :]
    result = jnp.einsum("bkij,nbkj->nbi", tile_set, picked, precision=lax.Precision.HIGHEST)
    return result.reshape(extended.shape[0], -1)


def scaled_inverse(tile_set, tile_cols):
    block_count = tile_set.shape[0]
    own_mask = (tile_cols == jnp.arange(block_count, dtype=jnp.int32)[:, None]).astype(tile_set.dtype)
    diagonal = jnp.sum(own_mask[:, :, None] * jnp.diagonal(tile_set, axis1=2, axis2=3), axis=1)
    return (RELAXATION / diagonal).reshape(-1)


def pick_rows(vector, row_index):
    return vector[:, row_index]


def owner_extend(values, send_lists):
    to_lower = jax.vmap(pick_rows)(values, send_lists[:, 0])
    to_upper = jax.vmap(pick_rows)(values, send_lists[:, 1])
    nothing = jnp.zeros_like(to_lower[:1])
    from_lower = jnp.concatenate([nothing, to_upper[:-1]], axis=0)
    from_upper = jnp.concatenate([to_lower[1:], nothing], axis=0)
    return jnp.concatenate([values, from_lower, from_upper], axis=2)


def restrict_rows(values, weights, agg_map, coarse_count):
    return jax.ops.segment_sum((values * weights).T, agg_map, coarse_count).T


def prolong_rows(values, weights, agg_map):
    return weights * values[:, agg_map]


def inner_sum(first_vec, second_vec):
    return jnp.sum(first_vec * second_vec, axis=(0, 2))


def reference(right_side, fine_tiles, fine_columns, fine_sends, fine_weights, fine_groups,
              group_tiles, group_columns, group_sends, group_weights, group_groups,
              coarse_tiles, coarse_columns):
    owners = N_GRP * N_MEM
    fine_count = R0 // AGG1
    fine_set = fine_tiles.reshape(owners, NB0, 3, TILE, TILE)
    fine_cols = fine_columns.reshape(owners, NB0, 3)
    fine_lists = fine_sends.reshape(owners, 2, HALO0)
    fine_wts = fine_weights.reshape(owners, R0)
    fine_maps = fine_groups.reshape(owners, R0)
    group_set = group_tiles.reshape(N_GRP, NB1, 3, TILE, TILE)
    group_cols = group_columns.reshape(N_GRP, NB1, 3)
    group_lists = group_sends.reshape(N_GRP, 2, HALO1)
    group_wts = group_weights.reshape(N_GRP, ROWS1)
    group_maps = group_groups.reshape(N_GRP, ROWS1)
    fine_scale = jax.vmap(scaled_inverse)(fine_set, fine_cols)[:, None, :]
    group_scale = jax.vmap(scaled_inverse)(group_set, group_cols)[:, None, :]
    coarse_scale = scaled_inverse(coarse_tiles, coarse_columns)
    fine_restrict = jax.vmap(functools.partial(restrict_rows, coarse_count=fine_count))
    group_restrict = jax.vmap(functools.partial(restrict_rows, coarse_count=ROWS2))

    def fine_apply(values):
        return jax.vmap(tile_apply)(fine_set, fine_cols, owner_extend(values, fine_lists))

    def group_apply(values):
        return jax.vmap(tile_apply)(group_set, group_cols, owner_extend(values, group_lists))

    def vcycle(source):
        fine_iter = fine_scale * source
        fine_left = source - fine_apply(fine_iter)
        lowered = fine_restrict(fine_left, fine_wts, fine_maps)
        group_rhs = lowered.reshape(N_GRP, N_MEM, NRHS, fine_count).transpose(0, 2, 1, 3).reshape(N_GRP, NRHS, ROWS1)
        group_iter = group_scale * group_rhs
        group_left = group_rhs - group_apply(group_iter)
        coarse_part = group_restrict(group_left, group_wts, group_maps)
        coarse_rhs = coarse_part.transpose(1, 0, 2).reshape(NRHS, COARSE)
        coarse_iter = coarse_scale * coarse_rhs
        coarse_iter = coarse_iter + coarse_scale * (coarse_rhs - tile_apply(coarse_tiles, coarse_columns, coarse_iter))
        raised = coarse_iter.reshape(NRHS, N_GRP, ROWS2).transpose(1, 0, 2)
        group_iter = group_iter + jax.vmap(prolong_rows)(raised, group_wts, group_maps)
        group_iter = group_iter + group_scale * (group_rhs - group_apply(group_iter))
        spread = group_iter.reshape(N_GRP, NRHS, N_MEM, fine_count).transpose(0, 2, 1, 3).reshape(owners, NRHS, fine_count)
        fine_iter = fine_iter + jax.vmap(prolong_rows)(spread, fine_wts, fine_maps)
        return fine_iter + fine_scale * (source - fine_apply(fine_iter))

    residual = right_side.reshape(NRHS, owners, R0).transpose(1, 0, 2)
    solution = jnp.zeros_like(residual)
    precond = vcycle(residual)
    energy = inner_sum(residual, precond)
    direction = precond
    for iteration in range(ITERS):
        images = fine_apply(direction)
        step_size = (energy / inner_sum(direction, images))[None, :, None]
        solution = solution + step_size * direction
        residual = residual - step_size * images
        if iteration + 1 < ITERS:
            precond = vcycle(residual)
            fresh = inner_sum(residual, precond)
            direction = precond + (fresh / energy)[None, :, None] * direction
            energy = fresh
    solution = solution.transpose(1, 0, 2).reshape(NRHS, UNKNOWNS)
    residual = residual.transpose(1, 0, 2).reshape(NRHS, UNKNOWNS)
    return solution, residual
```

```python
import functools

import jax
import jax.numpy as jnp
from jax import lax
from jax.experimental import pallas as pl
from jax.experimental.pallas import tpu as pltpu
from jax.sharding import Mesh
from jax.sharding import PartitionSpec as P

TILE = 128
AGG1 = 8
AGG2 = 32
ALL = ("grp_0", "grp_1", "mem_0", "mem_1")
GRP = ("grp_0", "grp_1")
MEM = ("mem_0", "mem_1")
RELAXATION = 0.7
F32 = jnp.float32
BF16 = jnp.bfloat16
VMEM_SPEC = pl.BlockSpec(memory_space=pltpu.VMEM)
SMEM_SPEC = pl.BlockSpec(memory_space=pltpu.SMEM)
LIMIT = 24 * 1024 * 1024


def shape(dims, dtype=F32):
    return jax.ShapeDtypeStruct(tuple(dims), dtype)


def run(kernel, name, outs, args, smem=(), scratch=(), flops=4_000_000_000):
    specs = [SMEM_SPEC if i in smem else VMEM_SPEC for i in range(len(args))]
    return pl.pallas_call(
        kernel,
        name=name,
        out_shape=tuple(outs),
        in_specs=specs,
        out_specs=tuple(VMEM_SPEC for _ in outs),
        scratch_shapes=list(scratch),
        compiler_params=pltpu.CompilerParams(vmem_limit_bytes=LIMIT),
        cost_estimate=pl.CostEstimate(flops=flops, transcendentals=0, bytes_accessed=4_000_000),
    )(*args)


def halves(value):
    high = value.astype(BF16)
    low = (value - high.astype(F32)).astype(BF16)
    return high, low


def stacked(value):
    high, low = halves(value)
    return jnp.concatenate([high, low], axis=0)


def doubled(value):
    both = stacked(value)
    return jnp.concatenate([both, both], axis=1)


def joined(both):
    rows = both.shape[0] // 2
    return both[:rows] + both[rows:]


def dot_nt(left, right):
    return lax.dot_general(left, right, (((1,), (1,)), ((), ())), preferred_element_type=F32)


def dot_nn(left, right):
    return lax.dot_general(left, right, (((1,), (0,)), ((), ())), preferred_element_type=F32)


def select_nn(value, onehot):
    return joined(dot_nn(stacked(value), onehot))


def select_nt(value, onehot):
    return joined(dot_nt(stacked(value), onehot))


def fill_blocks(blocks, value, first=0):
    for i in range(value.shape[1] // TILE):
        blocks[first + i] = doubled(value[:, i * TILE : (i + 1) * TILE])


def tile_rows(columns, weights, blocks, store, count, unroll=4):
    def step(i, carry):
        for j in range(unroll):
            b = i * unroll + j
            acc = dot_nt(blocks[columns[b, 0]], weights[b * 3])
            acc += dot_nt(blocks[columns[b, 1]], weights[b * 3 + 1])
            acc += dot_nt(blocks[columns[b, 2]], weights[b * 3 + 2])
            store(b, joined(acc))
        return carry

    lax.fori_loop(0, count // unroll, step, 0)


def lane_block(b):
    return pl.ds(pl.multiple_of(b * TILE, TILE), TILE)


def halo_rows(columns, weights, halo_blocks, image, own_blocks):
    def step(b, carry):
        for k in (1, 2):
            col = columns[b, k]

            @pl.when(col >= own_blocks)
            def _():
                acc = dot_nt(halo_blocks[col - own_blocks], weights[b * 3 + k])
                image[:, lane_block(b)] += joined(acc)

        return carry

    lax.fori_loop(0, own_blocks, step, 0)


def diagonal_scale(columns, tiles, scale):
    count = tiles.shape[0]
    rows = lax.broadcasted_iota(jnp.int32, (TILE, TILE), 0)
    lanes = lax.broadcasted_iota(jnp.int32, (TILE, TILE), 1)
    eye = rows == lanes

    def diagonal(b, k):
        return jnp.sum(jnp.where(eye, tiles[b, k], 0.0), axis=0, keepdims=True)

    for b in range(count):
        here = slice(b * TILE, (b + 1) * TILE)
        scale[:, here] = diagonal(b, 0)
        for k in (1, 2):

            @pl.when(columns[b, k] == b)
            def _():
                scale[:, here] += diagonal(b, k)

    scale[...] = RELAXATION / scale[...]


def pack_tile(tile):
    high, low = halves(tile)
    return jnp.concatenate([high, low], axis=1)


def onehot_by_lane(index_row, rows):
    place = lax.broadcasted_iota(jnp.int32, (rows, index_row.shape[1]), 0)
    return jnp.where(place == index_row, 1.0, 0.0).astype(BF16)


def first_kernel(columns, tiles, sends, source, scale, start, low_out, high_out, picks):
    diagonal_scale(columns, tiles, scale)
    rows = picks.shape[0]
    chunk = 256
    for i in range(rows // chunk):
        place = lax.broadcasted_iota(jnp.int32, (chunk, sends.shape[1]), 0) + i * chunk
        picks[i * chunk : (i + 1) * chunk, :] = jnp.where(place == sends[...], 1.0, 0.0).astype(BF16)
    begin = scale[...] * source[...]
    start[...] = begin
    out = select_nn(begin, picks[...])
    width = low_out.shape[1]
    low_out[...] = out[:, :width]
    high_out[...] = out[:, width:]


def pack_fine_kernel(tiles, groups, weights, table):
    for b in range(tiles.shape[0]):
        for k in range(3):
            weights[b * 3 + k] = pack_tile(tiles[b, k])
    table[...] = onehot_by_lane(groups[...], table.shape[0])


def inner_kernel(columns, weights, value, image, blocks):
    own = value.shape[1] // TILE
    fill_blocks(blocks, value[...])
    zero = jnp.zeros(blocks.shape[1:], BF16)
    for i in range(own, blocks.shape[0]):
        blocks[i] = zero

    def store(b, row):
        image[:, lane_block(b)] = row

    tile_rows(columns, weights, blocks, store, own)


def group_setup_kernel(
    place, columns, tiles, sends, weights, groups, ccolumns, ctiles,
    scale, packed, picks, table, cscale, cpacked, edge_low, edge_high,
):
    diagonal_scale(columns, tiles, scale)
    for b in range(tiles.shape[0]):
        for k in range(3):
            packed[b * 3 + k] = pack_tile(tiles[b, k])
    picks[...] = onehot_by_lane(sends[...], picks.shape[0])
    table[...] = onehot_by_lane(groups[...], table.shape[0])
    diagonal_scale(ccolumns, ctiles, cscale)
    for t in range(2):
        row = place[2 + t]
        for k in range(3):
            cpacked[t * 3 + k] = pack_tile(ctiles[row, k])
    length = weights.shape[1]
    numbers = groups[...].astype(F32)
    lines = lax.broadcasted_iota(jnp.int32, (8, length), 0)
    facts = jnp.where(lines == 0, weights[...], jnp.where(lines == 1, numbers, 0.0))
    picked = select_nn(facts, picks[...])
    half = edge_low.shape[1]
    edge_low[...] = picked[:, :half]
    edge_high[...] = picked[:, half:]


def group_edges_kernel(place, weights, groups, from_low, from_high, wide_weights, raise_table):
    length = weights.shape[1]
    half = from_low.shape[1]
    wide_weights[:, :length] = weights[...]
    wide_weights[:, length : length + half] = from_low[0:1, :]
    wide_weights[:, length + half :] = from_high[0:1, :]
    base = place[4]
    rows = raise_table.shape[0]
    raise_table[:, :length] = onehot_by_lane(groups[...] + base, rows)
    low = from_low[1:2, :].astype(jnp.int32) + (base - 64)
    high = from_high[1:2, :].astype(jnp.int32) + (base + 64)
    raise_table[:, length : length + half] = onehot_by_lane(low, rows)
    raise_table[:, length + half :] = onehot_by_lane(high, rows)


def restrict_kernel(
    columns, weights, image, from_low, from_high, source, agg_weights, table, extra, lowered,
    blocks, total,
):
    own = source.shape[1] // TILE
    fill_blocks(blocks, from_low[...])
    fill_blocks(blocks, from_high[...], from_low.shape[1] // TILE)
    total[...] = image[...]
    halo_rows(columns, weights, blocks, total, own)
    left = (source[...] - total[...]) * agg_weights[...]
    coarse = select_nt(left, table[...])
    width = table.shape[0]
    for i in range(lowered.shape[0]):
        lowered[i, :, :width] = coarse
        lowered[i, :, width:] = extra[...]


def group_start_kernel(gathered, scale, picks, group_rhs, start, low_out, high_out, extra):
    members = gathered.shape[0]
    width = group_rhs.shape[1] // members
    total = gathered[0, :, width:]
    for i in range(members):
        group_rhs[:, i * width : (i + 1) * width] = gathered[i, :, :width]
        if i:
            total += gathered[i, :, width:]
    extra[...] = total
    begin = scale[...] * group_rhs[...]
    start[...] = begin
    out = select_nn(begin, picks[...])
    half = low_out.shape[1]
    low_out[...] = out[:, :half]
    high_out[...] = out[:, half:]


def group_restrict_kernel(
    columns, weights, image, from_low, from_high, source, agg_weights, table, extra, payload,
    blocks, total,
):
    own = source.shape[1] // TILE
    fill_blocks(blocks, from_low[...])
    fill_blocks(blocks, from_high[...], from_low.shape[1] // TILE)
    total[...] = image[...]
    halo_rows(columns, weights, blocks, total, own)
    left = (source[...] - total[...]) * agg_weights[...]
    coarse = select_nt(left, table[...])
    half = coarse.shape[0] // 2
    packed = jnp.concatenate([coarse[:half, :64], coarse[half:, :64]], axis=1)
    lanes = lax.broadcasted_iota(jnp.int32, (8, TILE), 1)
    sums = jnp.zeros((8, TILE), F32)
    for j in range(4):
        part = jnp.where(lanes < 2, extra[8 * j : 8 * j + 8, :], 0.0)
        sums += pltpu.roll(part, 2 * j, 1) if j else part
    message = jnp.concatenate([packed, sums], axis=0)
    for i in range(payload.shape[0]):
        payload[i] = message


def coarse_kernel(
    place, ccolumns, columns, gathered, cscale, cpacked, own_start, from_low, from_high,
    group_rhs, scale, packed, wide_weights, raise_table, fine_start, fine_weights, fine_table,
    picks, fine_next, low_out, high_out, totals, blocks,
):
    lanes = lax.broadcasted_iota(jnp.int32, (16, TILE), 1)

    def block(t):
        first = gathered[2 * t, :16, :]
        second = gathered[2 * t + 1, :16, :]
        top = jnp.where(lanes < 64, first, pltpu.roll(second, 64, 1))
        bottom = jnp.where(lanes < 64, pltpu.roll(first, 64, 1), second)
        return jnp.concatenate([top, bottom], axis=0)

    sums = gathered[0, 16:24, :]
    for i in range(1, gathered.shape[0]):
        sums += gathered[i, 16:24, :]
    totals[...] = jnp.concatenate(
        [sums] + [pltpu.roll(sums, TILE - 2 * j, 1) for j in range(1, 4)], axis=0
    )
    solved = []
    for t in range(2):
        row = place[2 + t]
        acc = jnp.zeros((64, TILE), F32)
        for k in range(3):
            col = ccolumns[row, k]
            acc += dot_nt(doubled(cscale[col] * block(col)), cpacked[t * 3 + k])
        mine = block(row)
        iterate = cscale[row] * mine
        solved.append(iterate + cscale[row] * (mine - joined(acc)))
    pair = jnp.concatenate(solved, axis=1)
    raised = select_nn(pair, raise_table[...]) * wide_weights[...]
    length = own_start.shape[1]
    half = from_low.shape[1]
    now = own_start[...] + raised[:, :length]
    fill_blocks(blocks, now)
    fill_blocks(blocks, from_low[...] + raised[:, length : length + half], length // TILE)
    fill_blocks(
        blocks, from_high[...] + raised[:, length + half :], (length + half) // TILE
    )
    member = place[1]
    iterate_rows = []
    for j in range(2):
        b = member * 2 + j
        acc = dot_nt(blocks[columns[b, 0]], packed[b * 3])
        acc += dot_nt(blocks[columns[b, 1]], packed[b * 3 + 1])
        acc += dot_nt(blocks[columns[b, 2]], packed[b * 3 + 2])
        at = lane_block(b)
        mine = own_start[:, at]
        twice = blocks[b]
        current = twice[:32, :TILE].astype(F32) + twice[32:, :TILE].astype(F32)
        iterate_rows.append(current + scale[:, at] * (group_rhs[:, at] - joined(acc)))
    spread = jnp.concatenate(iterate_rows, axis=1)
    following = fine_start[...] + fine_weights[...] * select_nn(spread, fine_table[...])
    fine_next[...] = following
    out = select_nn(following, picks[...])
    width = low_out.shape[1]
    low_out[...] = out[:, :width]
    high_out[...] = out[:, width:]


def smooth_kernel(
    columns, weights, image, from_low, from_high, iterate, scale, source, picks,
    smoothed, low_out, high_out, blocks, total,
):
    own = source.shape[1] // TILE
    fill_blocks(blocks, from_low[...])
    fill_blocks(blocks, from_high[...], from_low.shape[1] // TILE)
    total[...] = image[...]
    halo_rows(columns, weights, blocks, total, own)
    value = iterate[...] + scale[...] * (source[...] - total[...])
    smoothed[...] = value
    out = select_nn(value, picks[...])
    width = low_out.shape[1]
    low_out[...] = out[:, :width]
    high_out[...] = out[:, width:]


def image_kernel(
    columns, weights, image, from_low, from_high, scale, residual, value, picks,
    product, start, low_out, high_out, extra, blocks,
):
    own = value.shape[1] // TILE
    fill_blocks(blocks, from_low[...])
    fill_blocks(blocks, from_high[...], from_low.shape[1] // TILE)
    product[...] = image[...]
    halo_rows(columns, weights, blocks, product, own)
    total = product[...]
    begin = scale[...] * total
    start[...] = begin
    out = select_nn(begin, picks[...])
    width = low_out.shape[1]
    low_out[...] = out[:, :width]
    high_out[...] = out[:, width:]
    energy = jnp.sum(residual[...] * value[...], axis=1, keepdims=True)
    curve = jnp.sum(value[...] * total, axis=1, keepdims=True)
    lanes = lax.broadcasted_iota(jnp.int32, (32, TILE), 1)
    extra[...] = jnp.where(lanes == 0, energy, jnp.where(lanes == 1, curve, 0.0))


def last_image_kernel(
    columns, weights, image, from_low, from_high, totals, residual, value, product, second,
    next_residual, next_value, next_product, partial, blocks, total,
):
    own = value.shape[1] // TILE
    fill_blocks(blocks, from_low[...])
    fill_blocks(blocks, from_high[...], from_low.shape[1] // TILE)
    total[...] = image[...]
    halo_rows(columns, weights, blocks, total, own)
    step = totals[:, 0:1] / totals[:, 1:2]
    left = residual[...] - step * product[...]
    fresh = value[...] - step * second[...]
    reach = product[...] - step * total[...]
    next_residual[...] = left
    next_value[...] = fresh
    next_product[...] = reach
    new = jnp.sum(left * fresh, axis=1, keepdims=True)
    own_curve = jnp.sum(fresh * reach, axis=1, keepdims=True)
    cross = jnp.sum(fresh * product[...] + value[...] * reach, axis=1, keepdims=True)
    lanes = lax.broadcasted_iota(jnp.int32, (32, TILE), 1)
    partial[...] = jnp.where(
        lanes == 0, new, jnp.where(lanes == 1, own_curve, jnp.where(lanes == 2, cross, 0.0))
    )


def sum_copies_kernel(parts, copies):
    total = parts[0]
    for i in range(1, parts.shape[0]):
        total += parts[i]
    for i in range(copies.shape[0]):
        copies[i] = total


def final_kernel(
    parts, totals, value, product, left, fresh, reach, solution, residual,
):
    sums = parts[0]
    for i in range(1, parts.shape[0]):
        sums += parts[i]
    energy = totals[:, 0:1]
    curve = totals[:, 1:2]
    step = energy / curve
    new = sums[:, 0:1]
    ratio = new / energy
    second_curve = sums[:, 1:2] + ratio * sums[:, 2:3] + ratio * ratio * curve
    second_step = new / second_curve
    solution[...] = step * value[...] + second_step * (fresh[...] + ratio * value[...])
    residual[...] = left[...] - second_step * (reach[...] + ratio * product[...])


def neighbours(low_out, high_out, axes):
    count = lax.axis_size(axes)
    up = [(i, i + 1) for i in range(count - 1)]
    down = [(b, a) for a, b in up]
    return lax.ppermute(high_out, axes, up), lax.ppermute(low_out, axes, down)


def exchanged(copies, axes):
    return lax.all_to_all(copies, axes, split_axis=0, concat_axis=0, tiled=True)


def shards(
    right_side,
    fine_tiles,
    fine_columns,
    fine_sends,
    fine_weights,
    fine_groups,
    group_tiles,
    group_columns,
    group_sends,
    group_weights,
    group_groups,
    coarse_tiles,
    coarse_columns,
):
    rhs, length = right_side.shape
    fine_count = length // AGG1
    group_length = group_weights.shape[0]
    share = group_length // AGG2
    members = lax.axis_size(MEM)
    group_total = lax.axis_size(GRP)
    fine_half = fine_sends.shape[1]
    group_half = group_sends.shape[1]
    fine_halo = 2 * fine_half // TILE
    group_halo = 2 * group_half // TILE
    fine_blocks = length // TILE
    group_blocks = group_length // TILE
    coarse_blocks = coarse_tiles.shape[0]

    fine_sends = fine_sends.reshape(1, -1)
    group_sends = group_sends.reshape(1, -1)
    fine_weights = fine_weights.reshape(1, -1)
    fine_groups = fine_groups.reshape(1, -1)
    group_weights = group_weights.reshape(1, -1)
    group_groups = group_groups.reshape(1, -1)

    grp = lax.axis_index(GRP)
    mem = lax.axis_index(MEM)
    row_a = jnp.maximum((grp - 1) // 2, 0)
    row_b = jnp.minimum(row_a + 1, coarse_blocks - 1)
    place = jnp.stack([grp, mem, row_a, row_b, grp * share - row_a * TILE]).astype(jnp.int32)

    block_scratch = pltpu.VMEM((fine_halo, 2 * rhs, 2 * TILE), BF16)
    group_block_scratch = pltpu.VMEM((group_halo, 2 * rhs, 2 * TILE), BF16)
    total_scratch = pltpu.VMEM((rhs, length), F32)
    edge = shape((rhs, fine_half))
    group_edge = shape((rhs, group_half))
    field = shape((rhs, length))

    fine_scale, fine_start, low_out, high_out, fine_picks = run(
        first_kernel, "first",
        [shape((1, length)), field, edge, edge, shape((length, 2 * fine_half), BF16)],
        (fine_columns, fine_tiles, fine_sends, right_side), smem=(0,),
    )
    before, after = neighbours(low_out, high_out, ALL)
    fine_packed, fine_table = run(
        pack_fine_kernel, "pack_fine",
        [shape((3 * fine_blocks, TILE, 2 * TILE), BF16), shape((fine_count, length), BF16)],
        (fine_tiles, fine_groups),
    )

    (group_scale, group_packed, group_picks, group_table, coarse_scale, coarse_packed,
     edge_low, edge_high) = run(
        group_setup_kernel, "group_setup",
        [
            shape((1, group_length)),
            shape((3 * group_blocks, TILE, 2 * TILE), BF16),
            shape((group_length, 2 * group_half), BF16),
            shape((TILE, group_length), BF16),
            shape((1, coarse_blocks * TILE)),
            shape((6, TILE, 2 * TILE), BF16),
            shape((8, group_half)),
            shape((8, group_half)),
        ],
        (place, group_columns, group_tiles, group_sends, group_weights, group_groups,
         coarse_columns, coarse_tiles),
        smem=(0, 1, 6),
    )
    coarse_scale = coarse_scale.reshape(coarse_blocks, 1, TILE)
    edge_before, edge_after = neighbours(edge_low, edge_high, GRP)
    wide_weights, raise_table = run(
        group_edges_kernel, "group_edges",
        [shape((1, group_length + 2 * group_half)),
         shape((2 * TILE, group_length + 2 * group_half), BF16)],
        (place, group_weights, group_groups, edge_before, edge_after), smem=(0,),
    )

    def inner(value):
        return run(
            inner_kernel, "inner", [field], (fine_columns, fine_packed, value), smem=(0,),
            scratch=[pltpu.VMEM((fine_blocks + fine_halo, 2 * rhs, 2 * TILE), BF16)],
        )[0]

    def group_inner(value):
        return run(
            inner_kernel, "group_inner", [field], (group_columns, group_packed, value), smem=(0,),
            scratch=[pltpu.VMEM((group_blocks + group_halo, 2 * rhs, 2 * TILE), BF16)],
        )[0]

    def vcycle(source, fine_start, before, after, extra):
        image = inner(fine_start)
        lowered = run(
            restrict_kernel, "restrict", [shape((members, rhs, fine_count + TILE))],
            (fine_columns, fine_packed, image, before, after, source, fine_weights, fine_table,
             extra),
            smem=(0,), scratch=[block_scratch, total_scratch],
        )[0]
        gathered = exchanged(lowered, MEM)
        group_rhs, group_start, low_out, high_out, extra = run(
            group_start_kernel, "group_start",
            [field, field, group_edge, group_edge, shape((rhs, TILE))],
            (gathered, group_scale, group_picks),
        )
        g_before, g_after = neighbours(low_out, high_out, GRP)
        image = group_inner(group_start)
        payload = run(
            group_restrict_kernel, "group_restrict", [shape((group_total, 24, TILE))],
            (group_columns, group_packed, image, g_before, g_after, group_rhs, group_weights,
             group_table, extra),
            smem=(0,), scratch=[group_block_scratch, total_scratch],
        )[0]
        gathered = exchanged(payload, GRP)
        fine_next, low_out, high_out, totals = run(
            coarse_kernel, "coarse", [field, edge, edge, shape((rhs, TILE))],
            (place, coarse_columns, group_columns, gathered, coarse_scale, coarse_packed,
             group_start, g_before, g_after, group_rhs, group_scale, group_packed, wide_weights,
             raise_table, fine_start, fine_weights, fine_table, fine_picks),
            smem=(0, 1, 2),
            scratch=[pltpu.VMEM((group_blocks + group_halo, 2 * rhs, 2 * TILE), BF16)],
        )
        before, after = neighbours(low_out, high_out, ALL)
        image = inner(fine_next)
        smoothed, low_out, high_out = run(
            smooth_kernel, "smooth", [field, edge, edge],
            (fine_columns, fine_packed, image, before, after, fine_next, fine_scale, source,
             fine_picks),
            smem=(0,), scratch=[block_scratch, total_scratch],
        )
        before, after = neighbours(low_out, high_out, ALL)
        image = inner(smoothed)
        return smoothed, image, before, after, totals

    nothing = jnp.zeros((rhs, TILE), F32)
    value, image, before, after, _ = vcycle(right_side, fine_start, before, after, nothing)
    product, start, low_out, high_out, extra = run(
        image_kernel, "image", [field, field, edge, edge, shape((rhs, TILE))],
        (fine_columns, fine_packed, image, before, after, fine_scale, right_side, value,
         fine_picks),
        smem=(0,), scratch=[block_scratch],
    )
    before, after = neighbours(low_out, high_out, ALL)
    second, image, before, after, totals = vcycle(product, start, before, after, extra)
    left, fresh, reach, partial = run(
        last_image_kernel, "last_image", [field, field, field, shape((rhs, TILE))],
        (fine_columns, fine_packed, image, before, after, totals, right_side, value, product,
         second),
        smem=(0,), scratch=[block_scratch, total_scratch],
    )
    copies = jnp.broadcast_to(partial, (members, rhs, TILE))
    copies = run(
        sum_copies_kernel, "sum_copies", [shape((group_total, rhs, TILE))],
        (exchanged(copies, MEM),),
    )[0]
    parts = exchanged(copies, GRP)
    solution, residual = run(
        final_kernel, "final", [field, field],
        (parts, totals, value, product, left, fresh, reach),
    )
    return solution, residual


def solution(mesh):
    finer = Mesh(mesh.devices.reshape(8, 4, 4, 2), ALL)
    return jax.shard_map(
        shards,
        mesh=finer,
        in_specs=(
            P(None, ALL),
            P(ALL, None, None, None),
            P(ALL, None),
            P(ALL, None),
            P(ALL),
            P(ALL),
            P(GRP, None, None, None),
            P(GRP, None),
            P(GRP, None),
            P(GRP),
            P(GRP),
            P(),
            P(),
        ),
        out_specs=(P(None, ALL), P(None, ALL)),
        check_vma=False,
    )
```

```python
import functools

import jax
import jax.numpy as jnp
from jax import lax
from jax.experimental import pallas as pl
from jax.experimental.pallas import tpu as pltpu
from jax.sharding import Mesh
from jax.sharding import PartitionSpec as P

TILE = 128
AGG1 = 8
AGG2 = 32
ALL = ("grp_0", "grp_1", "mem_0", "mem_1")
GRP = ("grp_0", "grp_1")
MEM = ("mem_0", "mem_1")
RELAXATION = 0.7
F32 = jnp.float32
BF16 = jnp.bfloat16
VMEM_SPEC = pl.BlockSpec(memory_space=pltpu.VMEM)
SMEM_SPEC = pl.BlockSpec(memory_space=pltpu.SMEM)
HBM_SPEC = pl.BlockSpec(memory_space=pltpu.HBM)
CHUNKS = 8
LIMIT = 24 * 1024 * 1024


def shape(dims, dtype=F32):
    return pltpu.VMEM(tuple(dims), dtype)


def hbm(dims, dtype=F32):
    return jax.ShapeDtypeStruct(tuple(dims), dtype)


def scalars(count):
    return pltpu.SMEM((count,), jnp.int32)


def run(
    kernel, name, outs, args, smem=(), hbm_args=(), scratch=(), smem_outs=(), flops=4_000_000_000
):
    specs = [
        SMEM_SPEC if i in smem else HBM_SPEC if i in hbm_args else VMEM_SPEC
        for i in range(len(args))
    ]
    return pl.pallas_call(
        kernel,
        name=name,
        out_shape=tuple(outs),
        in_specs=specs,
        out_specs=tuple(SMEM_SPEC if i in smem_outs else VMEM_SPEC for i in range(len(outs))),
        scratch_shapes=list(scratch),
        compiler_params=pltpu.CompilerParams(vmem_limit_bytes=LIMIT),
        cost_estimate=pl.CostEstimate(flops=flops, transcendentals=0, bytes_accessed=4_000_000),
    )(*args)


def halves(value):
    high = value.astype(BF16)
    low = (value - high.astype(F32)).astype(BF16)
    return high, low


def stacked(value):
    high, low = halves(value)
    return jnp.concatenate([high, low], axis=0)


def doubled(value):
    both = stacked(value)
    return jnp.concatenate([both, both], axis=1)


def joined(both):
    rows = both.shape[0] // 2
    return both[:rows] + both[rows:]


def dot_nt(left, right):
    return lax.dot_general(left, right, (((1,), (1,)), ((), ())), preferred_element_type=F32)


def dot_nn(left, right):
    return lax.dot_general(left, right, (((1,), (0,)), ((), ())), preferred_element_type=F32)


def select_nn(value, onehot):
    return joined(dot_nn(stacked(value), onehot))


def select_nt(value, onehot):
    return joined(dot_nt(stacked(value), onehot))


def fill_blocks(blocks, value, first=0):
    for i in range(value.shape[1] // TILE):
        blocks[first + i] = doubled(value[:, i * TILE : (i + 1) * TILE])


def lane_block(b):
    return pl.ds(pl.multiple_of(b * TILE, TILE), TILE)


def tile_rows(columns, weights, blocks, diagonal, value, store, count, unroll=4):
    def step(i, carry):
        for j in range(unroll):
            b = i * unroll + j
            acc = dot_nn(blocks[columns[0, b]], weights[b * 3])
            acc += dot_nn(blocks[columns[1, b]], weights[b * 3 + 1])
            acc += dot_nn(blocks[columns[2, b]], weights[b * 3 + 2])
            at = lane_block(b)
            store(at, joined(acc) + diagonal[:, at] * value[:, at])
        return carry

    lax.fori_loop(0, count // unroll, step, 0)


def own_blocks(blocks, value):
    own = value.shape[1] // TILE
    fill_blocks(blocks, value[...])
    zero = jnp.zeros(blocks.shape[1:], BF16)
    for i in range(own, blocks.shape[0]):
        blocks[i] = zero


def halo_products(place, spot, visits, weights, near, far, blocks):
    halos = blocks.shape[0]
    width = halos // 2
    fill_blocks(blocks.at[pl.ds(place[spot] * width, width)], near[...])
    fill_blocks(blocks.at[pl.ds((1 - place[spot]) * width, width)], far[...])
    found = []
    for i in range(2 * halos):
        acc = dot_nn(blocks[i % halos], weights[visits[2 * halos + i]])
        found.append((lane_block(visits[i]), joined(acc)))
    return found


def note_visits(columns, visits, own, halos):
    for i in range(2 * halos):
        visits[i] = 0
        visits[2 * halos + i] = 3 * own
    for b in range(own):
        for k in (1, 2):
            col = columns[k, b]

            @pl.when(col >= own)
            def _():
                at = (k - 1) * halos + col - own
                visits[at] = b
                visits[2 * halos + at] = 3 * b + k


def fetch(source, target, sems, chunks=CHUNKS):
    step = source.shape[0] // chunks
    copies = []
    for i in range(chunks):
        part = pl.ds(i * step, step)
        copies.append(pltpu.make_async_copy(source.at[part], target.at[part], sems.at[i]))
        copies[-1].start()
    return copies


def diagonal_scale(columns, tiles, scale, first, rows):
    lines = lax.broadcasted_iota(jnp.int32, (TILE, TILE), 0)
    lanes = lax.broadcasted_iota(jnp.int32, (TILE, TILE), 1)
    eye = lines == lanes

    def diagonal(b, k):
        return jnp.sum(jnp.where(eye, tiles[b, k], 0.0), axis=0, keepdims=True)

    for b in rows:
        here = slice(b * TILE, (b + 1) * TILE)
        mine = diagonal(b, 0)
        if first is not None:
            first[:, here] = mine
        scale[:, here] = mine
        for k in (1, 2):

            @pl.when(columns[k, b] == b)
            def _():
                scale[:, here] += diagonal(b, k)


def chunk_rows(i, count):
    step = count // CHUNKS
    return range(i * step, (i + 1) * step)


def pack_tile(tile):
    high, low = halves(tile.T)
    return jnp.concatenate([high, low], axis=0)


def pack_tiles(tiles, packed, which):
    rows = lax.broadcasted_iota(jnp.int32, (TILE, TILE), 0)
    lanes = lax.broadcasted_iota(jnp.int32, (TILE, TILE), 1)
    for b in which:
        packed[b * 3] = pack_tile(jnp.where(rows == lanes, 0.0, tiles[b, 0]))
        packed[b * 3 + 1] = pack_tile(tiles[b, 1])
        packed[b * 3 + 2] = pack_tile(tiles[b, 2])


def onehot_by_lane(index_row, rows):
    place = lax.broadcasted_iota(jnp.int32, (rows, index_row.shape[1]), 0)
    return jnp.where(place == index_row, 1.0, 0.0).astype(BF16)


def fill_picks(flag, sends, picks):
    up = flag == 1
    near = jnp.where(up, sends[1:2, :], sends[0:1, :])
    far = jnp.where(up, sends[0:1, :], sends[1:2, :])
    chosen = jnp.concatenate([near, far], axis=1)
    chunk = 256
    for i in range(picks.shape[0] // chunk):
        place = lax.broadcasted_iota(jnp.int32, (chunk, chosen.shape[1]), 0) + i * chunk
        picks[i * chunk : (i + 1) * chunk, :] = jnp.where(place == chosen, 1.0, 0.0).astype(BF16)


def put_pair(out, near, far):
    width = near.shape[1]
    near[...] = out[:, :width]
    far[...] = out[:, width:]


def pick_correction(out, part, picks, at):
    return out + joined(dot_nn(stacked(part), picks[at, :]))


def compact(wide, count):
    lanes = lax.broadcasted_iota(jnp.int32, (8, TILE), 1)
    sums = jnp.zeros((8, TILE), F32)
    for j in range(4):
        part = jnp.where(lanes < count, wide[8 * j : 8 * j + 8, :], 0.0)
        sums += pltpu.roll(part, count * j, 1) if j else part
    return sums


def spread_rows(sums, count):
    return jnp.concatenate(
        [sums] + [pltpu.roll(sums, TILE - count * j, 1) for j in range(1, 4)], axis=0
    )


def lane_columns(parts):
    lanes = lax.broadcasted_iota(jnp.int32, (32, TILE), 1)
    out = jnp.zeros((32, TILE), F32)
    for i, part in enumerate(parts):
        out = jnp.where(lanes == i, part, out)
    return out


def row_sum(value):
    return jnp.sum(value, axis=1, keepdims=True)


def copy_scalars(source, target):
    for k in range(source.shape[0]):
        for b in range(source.shape[1]):
            target[k, b] = source[k, b]


def first_kernel(
    place, columns, tiles_hbm, sends_hbm, source_hbm, *rest, lines,
):
    lines_hbm = rest[:lines]
    (scale, diagonal, start, near, far, picks, tiles, source, place_out, columns_out) = rest[
        lines : lines + 10
    ]
    kept = rest[lines + 10 : 2 * lines + 10]
    sends, sems = rest[2 * lines + 10 :]
    count = tiles.shape[0]
    early = pltpu.make_async_copy(sends_hbm, sends, sems.at[CHUNKS])
    early.start()
    copies = fetch(tiles_hbm, tiles, sems)
    others = [pltpu.make_async_copy(source_hbm, source, sems.at[CHUNKS + 1])]
    for i in range(lines):
        others.append(pltpu.make_async_copy(lines_hbm[i], kept[i], sems.at[CHUNKS + 2 + i]))
    for copy in others:
        copy.start()
    for i in range(place.shape[0]):
        place_out[i] = place[i]
    copy_scalars(columns, columns_out)
    early.wait()
    fill_picks(place[5], sends, picks)
    for i, copy in enumerate(copies):
        copy.wait()
        diagonal_scale(columns, tiles, scale, diagonal, chunk_rows(i, count))
    for copy in others:
        copy.wait()
    scale[...] = RELAXATION / scale[...]
    begin = scale[...] * source[...]
    start[...] = begin
    put_pair(select_nn(begin, picks[...]), near, far)


def pack_fine_kernel(columns, tiles, groups, packed, table, visits):
    own = tiles.shape[0]
    pack_tiles(tiles, packed, range(own))
    packed[3 * own] = jnp.zeros(packed.shape[1:], BF16)
    table[...] = onehot_by_lane(groups[...], table.shape[0])
    note_visits(columns, visits, own, 4)


def group_setup_kernel(
    place, columns, tiles_hbm, sends, weights, groups, ccolumns, ctiles_hbm,
    scale, diagonal, packed, picks, table, cscale, cpacked, edge_near, edge_far, visits,
    columns_out, ccolumns_out, tiles, ctiles, cline, sems, csems,
):
    count = tiles.shape[0]
    copy_scalars(columns, columns_out)
    copy_scalars(ccolumns, ccolumns_out)
    copies = fetch(tiles_hbm, tiles, sems)
    ccopies = fetch(ctiles_hbm, ctiles, csems)
    fill_picks(place[6], sends, picks)
    table[...] = onehot_by_lane(groups[...], table.shape[0])
    length = weights.shape[1]
    numbers = groups[...].astype(F32)
    lines = lax.broadcasted_iota(jnp.int32, (8, length), 0)
    facts = jnp.where(lines == 0, weights[...], jnp.where(lines == 1, numbers, 0.0))
    put_pair(select_nn(facts, picks[...]), edge_near, edge_far)
    note_visits(columns, visits, count, 2)
    for i, copy in enumerate(copies):
        copy.wait()
        diagonal_scale(columns, tiles, scale, diagonal, chunk_rows(i, count))
        pack_tiles(tiles, packed, chunk_rows(i, count))
    packed[3 * count] = jnp.zeros(packed.shape[1:], BF16)
    scale[...] = RELAXATION / scale[...]
    blocks = ctiles.shape[0]
    for i, copy in enumerate(ccopies):
        copy.wait()
        diagonal_scale(ccolumns, ctiles, cline, None, chunk_rows(i, blocks))
    for b in range(blocks):
        cscale[b] = RELAXATION / cline[:, b * TILE : (b + 1) * TILE]
    for t in range(2):
        row = place[2 + t]
        for k in range(3):
            cpacked[t * 3 + k] = pack_tile(ctiles[row, k])


def group_edges_kernel(place, weights, groups, near, far, wide_weights, raise_table):
    length = weights.shape[1]
    half = near.shape[1]
    base = place[4]
    up = place[6]
    rows = raise_table.shape[0]
    wide_weights[:, :length] = weights[...]
    raise_table[:, :length] = onehot_by_lane(groups[...] + base, rows)
    low = jnp.where(up == 1, far[...], near[...])
    high = jnp.where(up == 1, near[...], far[...])
    wide_weights[:, length : length + half] = low[0:1, :]
    wide_weights[:, length + half :] = high[0:1, :]
    low_at = low[1:2, :].astype(jnp.int32) + (base - 64)
    high_at = high[1:2, :].astype(jnp.int32) + (base + 64)
    raise_table[:, length : length + half] = onehot_by_lane(low_at, rows)
    raise_table[:, length + half :] = onehot_by_lane(high_at, rows)


def inner_restrict_kernel(
    columns, weights, diagonal, value, source, agg_weights, table, coarse, blocks, left
):
    own_blocks(blocks, value)

    def store(at, row):
        left[:, at] = (source[:, at] - row) * agg_weights[:, at]

    tile_rows(columns, weights, blocks, diagonal, value, store, value.shape[1] // TILE)
    coarse[...] = select_nt(left[...], table[...])


def restrict_kernel(
    place, visits, weights, coarse, near, far, agg_weights, table, *rest, spot, after
):
    rest = rest[after:]
    lowered, blocks = rest[-2:]
    out = coarse[...]
    for at, part in halo_products(place, spot, visits, weights, near, far, blocks):
        out -= joined(dot_nt(stacked(part * agg_weights[:, at]), table[:, at]))
    if len(rest) == 3:
        lines = compact(rest[0][...], 2)
        out = jnp.concatenate(
            [out, jnp.concatenate([lines, jnp.zeros_like(lines)], axis=1)], axis=0
        )
    for i in range(lowered.shape[0]):
        lowered[i] = out


def group_start_kernel(gathered, scale, picks, group_rhs, start, near, far, *extra):
    members = gathered.shape[0]
    width = group_rhs.shape[1] // members
    for i in range(members):
        group_rhs[:, i * width : (i + 1) * width] = gathered[i, :32, :]
    if extra:
        total = gathered[0, 32:40, :TILE]
        for i in range(1, members):
            total += gathered[i, 32:40, :TILE]
        extra[0][...] = total
    begin = scale[...] * group_rhs[...]
    start[...] = begin
    put_pair(select_nn(begin, picks[...]), near, far)


def group_restrict_kernel(
    place, visits, weights, coarse, near, far, agg_weights, table, *rest, spot, after
):
    rest = rest[after:]
    payload, blocks = rest[-2:]
    out = coarse[...]
    for at, part in halo_products(place, spot, visits, weights, near, far, blocks):
        out -= joined(dot_nt(stacked(part * agg_weights[:, at]), table[:, at]))
    half = out.shape[0] // 2
    message = jnp.concatenate([out[:half, :64], out[half:, :64]], axis=1)
    if len(rest) == 3:
        message = jnp.concatenate([message, rest[0][...]], axis=0)
    for i in range(payload.shape[0]):
        payload[i] = message


def coarse_kernel(
    place, ccolumns, columns, gathered, cscale, cpacked, own_start, near, far,
    group_rhs, scale, diagonal, packed, wide_weights, raise_table, fine_start, fine_weights,
    fine_table, picks, *rest,
):
    blocks, current = rest[-2:]
    fine_next, near_out, far_out = rest[:3]
    lanes = lax.broadcasted_iota(jnp.int32, (16, TILE), 1)

    def block(t):
        first = gathered[2 * t, :16, :]
        second = gathered[2 * t + 1, :16, :]
        top = jnp.where(lanes < 64, first, pltpu.roll(second, 64, 1))
        bottom = jnp.where(lanes < 64, pltpu.roll(first, 64, 1), second)
        return jnp.concatenate([top, bottom], axis=0)

    if len(rest) == 6:
        sums = gathered[0, 16:24, :]
        for i in range(1, gathered.shape[0]):
            sums += gathered[i, 16:24, :]
        rest[3][...] = spread_rows(sums, 2)
    solved = []
    for t in range(2):
        row = place[2 + t]
        acc = jnp.zeros((64, TILE), F32)
        for k in range(3):
            col = ccolumns[k, row]
            acc += dot_nn(doubled(cscale[col] * block(col)), cpacked[t * 3 + k])
        mine = block(row)
        iterate = cscale[row] * mine
        solved.append(iterate + cscale[row] * (mine - joined(acc)))
    pair = jnp.concatenate(solved, axis=1)
    raised = select_nn(pair, raise_table[...]) * wide_weights[...]
    length = own_start.shape[1]
    half = near.shape[1]
    now = own_start[...] + raised[:, :length]
    current[...] = now
    fill_blocks(blocks, now)
    up = place[6]
    low = jnp.where(up == 1, far[...], near[...])
    high = jnp.where(up == 1, near[...], far[...])
    fill_blocks(blocks, low + raised[:, length : length + half], length // TILE)
    fill_blocks(blocks, high + raised[:, length + half :], (length + half) // TILE)
    member = place[1]
    iterate_rows = []
    for j in range(2):
        b = member * 2 + j
        acc = dot_nn(blocks[columns[0, b]], packed[b * 3])
        acc += dot_nn(blocks[columns[1, b]], packed[b * 3 + 1])
        acc += dot_nn(blocks[columns[2, b]], packed[b * 3 + 2])
        at = lane_block(b)
        mine = current[:, at]
        image = joined(acc) + diagonal[:, at] * mine
        iterate_rows.append(mine + scale[:, at] * (group_rhs[:, at] - image))
    spread = jnp.concatenate(iterate_rows, axis=1)
    following = fine_start[...] + fine_weights[...] * select_nn(spread, fine_table[...])
    fine_next[...] = following
    put_pair(select_nn(following, picks[...]), near_out, far_out)


def inner_smooth_kernel(
    columns, weights, diagonal, value, source, scale, picks, smoothed, out, blocks
):
    own_blocks(blocks, value)

    def store(at, row):
        smoothed[:, at] = value[:, at] + scale[:, at] * (source[:, at] - row)

    tile_rows(columns, weights, blocks, diagonal, value, store, value.shape[1] // TILE)
    out[...] = select_nn(smoothed[...], picks[...])


def smooth_kernel(
    place, visits, weights, inner, inner_out, near, far, scale, picks,
    smoothed, near_out, far_out, blocks,
):
    smoothed[...] = inner[...]
    out = inner_out[...]
    for at, part in halo_products(place, 5, visits, weights, near, far, blocks):
        change = -scale[:, at] * part
        smoothed[:, at] += change
        out = pick_correction(out, change, picks, at)
    put_pair(out, near_out, far_out)


def inner_image_kernel(
    columns, weights, diagonal, value, scale, residual, picks, product, out, sums, blocks
):
    own_blocks(blocks, value)

    def store(at, row):
        product[:, at] = row

    tile_rows(columns, weights, blocks, diagonal, value, store, value.shape[1] // TILE)
    image = product[...]
    out[...] = select_nn(scale[...] * image, picks[...])
    field = value[...]
    sums[...] = lane_columns([row_sum(residual[...] * field), row_sum(field * image)])


def image_kernel(
    place, visits, weights, inner, inner_out, inner_sums, near, far, scale, value, picks,
    product, start, near_out, far_out, sums, blocks,
):
    product[...] = inner[...]
    out = inner_out[...]
    curve = jnp.zeros((32, TILE), F32)
    for at, part in halo_products(place, 5, visits, weights, near, far, blocks):
        product[:, at] += part
        curve += value[:, at] * part
        out = pick_correction(out, scale[:, at] * part, picks, at)
    put_pair(out, near_out, far_out)
    start[...] = scale[...] * product[...]
    sums[...] = inner_sums[...] + lane_columns([jnp.zeros((32, 1), F32), row_sum(curve)])


def inner_last_kernel(
    columns, weights, diagonal, second, residual, value, product, image, sums, blocks,
):
    own_blocks(blocks, second)

    def store(at, row):
        image[:, at] = row

    tile_rows(columns, weights, blocks, diagonal, second, store, second.shape[1] // TILE)
    follow = image[...]
    field = second[...]
    along = product[...]
    zero = jnp.zeros((32, 1), F32)
    sums[...] = lane_columns(
        [
            zero,
            zero,
            row_sum(residual[...] * field),
            row_sum(along * field),
            row_sum(value[...] * follow + field * along),
            row_sum(field * follow),
        ]
    )


def last_kernel(
    place, visits, weights, inner, inner_sums, first_sums, near, far, value, second,
    image, copies, blocks,
):
    image[...] = inner[...]
    cross = jnp.zeros((32, TILE), F32)
    curve = jnp.zeros((32, TILE), F32)
    for at, part in halo_products(place, 5, visits, weights, near, far, blocks):
        image[:, at] += part
        cross += value[:, at] * part
        curve += second[:, at] * part
    zero = jnp.zeros((32, 1), F32)
    sums = inner_sums[...] + first_sums[...]
    sums += lane_columns([zero, zero, zero, zero, row_sum(cross), row_sum(curve)])
    message = compact(sums, 6)
    for i in range(copies.shape[0]):
        copies[i] = message


def sum_copies_kernel(parts, copies):
    total = parts[0]
    for i in range(1, parts.shape[0]):
        total += parts[i]
    for i in range(copies.shape[0]):
        copies[i] = total


def final_kernel(parts, start, value, product, second, image, solution, residual):
    small = parts[0]
    for i in range(1, parts.shape[0]):
        small += parts[i]
    sums = spread_rows(small, 6)
    energy, curve, along, across, cross, last = (sums[:, i : i + 1] for i in range(6))
    step = energy / curve
    new = step * (step * across - along)
    ratio = new / energy
    grown = 1.0 + ratio
    second_curve = grown * (grown * curve - step * cross) + step * step * last
    second_step = new / second_curve
    field = value[...]
    product_now = product[...]
    solution[...] = step * field + second_step * (grown * field - step * second[...])
    residual[...] = (start[...] - step * product_now) - second_step * (
        grown * product_now - step * image[...]
    )


def neighbours(near_out, far_out, axes):
    count = lax.axis_size(axes)
    near = [(i, i ^ 1) for i in range(count)]
    far = [(i, i + 1) for i in range(1, count - 1, 2)]
    far = far + [(b, a) for a, b in far]
    far_in = lax.ppermute(far_out, axes, far)
    return lax.ppermute(near_out, axes, near), far_in


def exchanged(copies, axes):
    return lax.all_to_all(copies, axes, split_axis=0, concat_axis=0, tiled=True)


def shards(
    right_side,
    fine_tiles,
    fine_columns,
    fine_sends,
    fine_weights,
    fine_groups,
    group_tiles,
    group_columns,
    group_sends,
    group_weights,
    group_groups,
    coarse_tiles,
    coarse_columns,
):
    rhs, length = right_side.shape
    fine_count = length // AGG1
    group_length = group_weights.shape[0]
    share = group_length // AGG2
    members = lax.axis_size(MEM)
    group_total = lax.axis_size(GRP)
    fine_half = fine_sends.shape[1]
    group_half = group_sends.shape[1]
    fine_halo = 2 * fine_half // TILE
    group_halo = 2 * group_half // TILE
    fine_blocks = length // TILE
    group_blocks = group_length // TILE
    coarse_blocks = coarse_tiles.shape[0]

    fine_weights = fine_weights.reshape(1, -1)
    fine_groups = fine_groups.reshape(1, -1)
    group_weights = group_weights.reshape(1, -1)
    group_groups = group_groups.reshape(1, -1)
    fine_columns = fine_columns.T
    group_columns = group_columns.T
    coarse_columns = coarse_columns.T

    grp = lax.axis_index(GRP)
    mem = lax.axis_index(MEM)
    row_a = jnp.maximum((grp - 1) // 2, 0)
    row_b = jnp.minimum(row_a + 1, coarse_blocks - 1)
    place = jnp.stack(
        [grp, mem, row_a, row_b, grp * share - row_a * TILE, 1 - mem % 2, 1 - grp % 2]
    ).astype(jnp.int32)

    def block_scratch(count):
        return pltpu.VMEM((count, 2 * rhs, 2 * TILE), BF16)

    edge = shape((rhs, fine_half))
    group_edge = shape((rhs, group_half))
    field = shape((rhs, length))
    line = shape((1, length))
    small = shape((rhs, TILE))
    picked = shape((rhs, 2 * fine_half))

    pinned = [
        pltpu.with_memory_space_constraint(x, pltpu.HBM)
        for x in (fine_tiles, fine_sends, right_side, fine_weights, fine_groups, group_weights,
                  group_groups, group_sends)
    ]
    group_tiles = pltpu.with_memory_space_constraint(group_tiles, pltpu.HBM)
    coarse_tiles = pltpu.with_memory_space_constraint(coarse_tiles, pltpu.HBM)
    (fine_scale, fine_diagonal, fine_start, near, far, fine_picks, fine_tiles, right_side,
     place, fine_columns, fine_weights, fine_groups, group_weights, group_groups,
     group_sends) = run(
        functools.partial(first_kernel, lines=5), "first",
        [line, line, field, edge, edge, shape((length, 2 * fine_half), BF16),
         shape(fine_tiles.shape), field, scalars(7), pltpu.SMEM(fine_columns.shape, jnp.int32),
         line, shape((1, length), jnp.int32), line, shape((1, group_length), jnp.int32),
         shape(group_sends.shape, jnp.int32)],
        [place, fine_columns] + pinned, smem=(0, 1), hbm_args=range(2, 10), smem_outs=(8, 9),
        scratch=[pltpu.VMEM(fine_sends.shape, jnp.int32),
                 pltpu.SemaphoreType.DMA((CHUNKS + 7,))],
    )
    near, far = neighbours(near, far, ALL)
    fine_packed, fine_table, fine_visits = run(
        pack_fine_kernel, "pack_fine",
        [shape((3 * fine_blocks + 1, 2 * TILE, TILE), BF16), shape((fine_count, length), BF16),
         scalars(4 * fine_halo)],
        (fine_columns, fine_tiles, fine_groups), smem=(0,), smem_outs=(2,),
    )

    (group_scale, group_diagonal, group_packed, group_picks, group_table, coarse_scale,
     coarse_packed, edge_near, edge_far, group_visits, group_columns, coarse_columns) = run(
        group_setup_kernel, "group_setup",
        [
            line,
            line,
            shape((3 * group_blocks + 1, 2 * TILE, TILE), BF16),
            shape((group_length, 2 * group_half), BF16),
            shape((TILE, group_length), BF16),
            shape((coarse_blocks, 1, TILE)),
            shape((6, 2 * TILE, TILE), BF16),
            shape((8, group_half)),
            shape((8, group_half)),
            scalars(4 * group_halo),
            pltpu.SMEM(group_columns.shape, jnp.int32),
            pltpu.SMEM(coarse_columns.shape, jnp.int32),
        ],
        (place, group_columns, group_tiles, group_sends, group_weights, group_groups,
         coarse_columns, coarse_tiles),
        smem=(0, 1, 6), smem_outs=(9, 10, 11), hbm_args=(2, 7),
        scratch=[pltpu.VMEM(group_tiles.shape, F32), pltpu.VMEM(coarse_tiles.shape, F32),
                 pltpu.VMEM((1, coarse_blocks * TILE), F32),
                 pltpu.SemaphoreType.DMA((CHUNKS,)), pltpu.SemaphoreType.DMA((CHUNKS,))],
    )
    edge_near, edge_far = neighbours(edge_near, edge_far, GRP)
    wide_weights, raise_table = run(
        group_edges_kernel, "group_edges",
        [shape((1, group_length + 2 * group_half)),
         shape((2 * TILE, group_length + 2 * group_half), BF16)],
        (place, group_weights, group_groups, edge_near, edge_far), smem=(0,),
    )

    def vcycle(source, fine_start, near, far, extra, first_after=(), second_after=()):
        carried = () if extra is None else (extra,)
        coarse = run(
            inner_restrict_kernel, "inner_restrict", [shape((rhs, fine_count))],
            (fine_columns, fine_packed, fine_diagonal, fine_start, source, fine_weights,
             fine_table),
            smem=(0,), scratch=[block_scratch(fine_blocks + fine_halo), pltpu.VMEM((rhs, length), F32)],
        )[0]
        lowered = run(
            functools.partial(restrict_kernel, spot=5, after=len(first_after)), "restrict",
            [shape((members, rhs + 8 * len(carried), fine_count))],
            (place, fine_visits, fine_packed, coarse, near, far, fine_weights, fine_table)
            + first_after + carried,
            smem=(0, 1), scratch=[block_scratch(fine_halo)],
        )[0]
        gathered = exchanged(lowered, MEM)
        group_rhs, group_start, near, far, *carried = run(
            group_start_kernel, "group_start",
            [field, field, group_edge, group_edge] + [shape((8, TILE)) for _ in carried],
            (gathered, group_scale, group_picks),
        )
        g_near, g_far = neighbours(near, far, GRP)
        coarse = run(
            inner_restrict_kernel, "group_inner", [shape((rhs, TILE))],
            (group_columns, group_packed, group_diagonal, group_start, group_rhs,
             group_weights, group_table),
            smem=(0,), scratch=[block_scratch(group_blocks + group_halo), pltpu.VMEM((rhs, length), F32)],
        )[0]
        payload = run(
            functools.partial(group_restrict_kernel, spot=6, after=len(second_after)),
            "group_restrict",
            [shape((group_total, 16 + 8 * len(carried), TILE))],
            (place, group_visits, group_packed, coarse, g_near, g_far, group_weights,
             group_table) + second_after + tuple(carried),
            smem=(0, 1), scratch=[block_scratch(group_halo)],
        )[0]
        gathered = exchanged(payload, GRP)
        fine_next, near, far, *totals = run(
            coarse_kernel, "coarse", [field, edge, edge] + [small for _ in carried],
            (place, coarse_columns, group_columns, gathered, coarse_scale, coarse_packed,
             group_start, g_near, g_far, group_rhs, group_scale, group_diagonal, group_packed,
             wide_weights, raise_table, fine_start, fine_weights, fine_table, fine_picks),
            smem=(0, 1, 2),
            scratch=[block_scratch(group_blocks + group_halo), pltpu.VMEM((rhs, length), F32)],
        )
        near, far = neighbours(near, far, ALL)
        inside, out = run(
            inner_smooth_kernel, "inner_smooth", [field, picked],
            (fine_columns, fine_packed, fine_diagonal, fine_next, source, fine_scale,
             fine_picks),
            smem=(0,), scratch=[block_scratch(fine_blocks + fine_halo)],
        )
        smoothed, near, far = run(
            smooth_kernel, "smooth", [field, edge, edge],
            (place, fine_visits, fine_packed, inside, out, near, far, fine_scale, fine_picks),
            smem=(0, 1), scratch=[block_scratch(fine_halo)],
        )
        near, far = neighbours(near, far, ALL)
        return smoothed, near, far, totals

    value, near, far, _ = vcycle(
        right_side, fine_start, near, far, None, (wide_weights,)
    )
    inside, out, sums = run(
        inner_image_kernel, "inner_image", [field, picked, small],
        (fine_columns, fine_packed, fine_diagonal, value, fine_scale, right_side, fine_picks),
        smem=(0,), scratch=[block_scratch(fine_blocks + fine_halo)],
    )
    product, start, near, far, sums = run(
        image_kernel, "image", [field, field, edge, edge, small],
        (place, fine_visits, fine_packed, inside, out, sums, near, far, fine_scale, value,
         fine_picks),
        smem=(0, 1), scratch=[block_scratch(fine_halo)],
    )
    near, far = neighbours(near, far, ALL)
    second, near, far, _ = vcycle(product, start, near, far, None)
    inside, more = run(
        inner_last_kernel, "inner_last", [field, small],
        (fine_columns, fine_packed, fine_diagonal, second, right_side, value, product),
        smem=(0,), scratch=[block_scratch(fine_blocks + fine_halo)],
    )
    image, copies = run(
        last_kernel, "last", [field, shape((members, 8, TILE))],
        (place, fine_visits, fine_packed, inside, more, sums, near, far, value, second),
        smem=(0, 1), scratch=[block_scratch(fine_halo)],
    )
    copies = run(
        sum_copies_kernel, "sum_copies", [shape((group_total, 8, TILE))],
        (exchanged(copies, MEM),),
    )[0]
    parts = exchanged(copies, GRP)
    solution, residual = run(
        final_kernel, "final", [hbm((rhs, length)), hbm((rhs, length))],
        (parts, right_side, value, product, second, image),
    )
    return solution, residual


def solution(mesh):
    finer = Mesh(mesh.devices.reshape(8, 4, 4, 2), ALL)
    return jax.shard_map(
        shards,
        mesh=finer,
        in_specs=(
            P(None, ALL),
            P(ALL, None, None, None),
            P(ALL, None),
            P(ALL, None),
            P(ALL),
            P(ALL),
            P(GRP, None, None, None),
            P(GRP, None),
            P(GRP, None),
            P(GRP),
            P(GRP),
            P(),
            P(),
        ),
        out_specs=(P(None, ALL), P(None, ALL)),
        check_vma=False,
    )
```

```python
import functools

import jax
import jax.numpy as jnp
from jax import lax
from jax.experimental import pallas as pl
from jax.experimental.pallas import tpu as pltpu
from jax.sharding import Mesh
from jax.sharding import PartitionSpec as P

TILE = 128
AGG1 = 8
AGG2 = 32
ALL = ("grp_0", "grp_1", "mem_0", "mem_1")
GRP = ("grp_0", "grp_1")
MEM = ("mem_0", "mem_1")
RELAXATION = 0.7
F32 = jnp.float32
BF16 = jnp.bfloat16
VMEM_SPEC = pl.BlockSpec(memory_space=pltpu.VMEM)
SMEM_SPEC = pl.BlockSpec(memory_space=pltpu.SMEM)
HBM_SPEC = pl.BlockSpec(memory_space=pltpu.HBM)
CHUNKS = 8
LIMIT = 24 * 1024 * 1024


def shape(dims, dtype=F32):
    return pltpu.VMEM(tuple(dims), dtype)


def hbm(dims, dtype=F32):
    return jax.ShapeDtypeStruct(tuple(dims), dtype)


def scalars(count):
    return pltpu.SMEM((count,), jnp.int32)


def run(
    kernel, name, outs, args, smem=(), hbm_args=(), scratch=(), smem_outs=(), flops=4_000_000_000
):
    specs = [
        SMEM_SPEC if i in smem else HBM_SPEC if i in hbm_args else VMEM_SPEC
        for i in range(len(args))
    ]
    return pl.pallas_call(
        kernel,
        name=name,
        out_shape=tuple(outs),
        in_specs=specs,
        out_specs=tuple(SMEM_SPEC if i in smem_outs else VMEM_SPEC for i in range(len(outs))),
        scratch_shapes=list(scratch),
        compiler_params=pltpu.CompilerParams(vmem_limit_bytes=LIMIT),
        cost_estimate=pl.CostEstimate(flops=flops, transcendentals=0, bytes_accessed=4_000_000),
    )(*args)


def halves(value):
    high = value.astype(BF16)
    low = (value - high.astype(F32)).astype(BF16)
    return high, low


def stacked(value):
    high, low = halves(value)
    return jnp.concatenate([high, low], axis=0)


def doubled(value):
    both = stacked(value)
    return jnp.concatenate([both, both], axis=1)


def joined(both):
    rows = both.shape[0] // 2
    return both[:rows] + both[rows:]


def dot_nt(left, right):
    return lax.dot_general(left, right, (((1,), (1,)), ((), ())), preferred_element_type=F32)


def dot_nn(left, right):
    return lax.dot_general(left, right, (((1,), (0,)), ((), ())), preferred_element_type=F32)


def select_nn(value, onehot):
    return joined(dot_nn(stacked(value), onehot))


def select_nt(value, onehot):
    return joined(dot_nt(stacked(value), onehot))


def fill_blocks(blocks, value, first=0):
    for i in range(value.shape[1] // TILE):
        blocks[first + i] = doubled(value[:, i * TILE : (i + 1) * TILE])


def lane_block(b):
    return pl.ds(pl.multiple_of(b * TILE, TILE), TILE)


def tile_rows(columns, weights, blocks, diagonal, value, store, count, unroll=4):
    def step(i, carry):
        for j in range(unroll):
            b = i * unroll + j
            acc = dot_nn(blocks[columns[0, b]], weights[b * 3])
            acc += dot_nn(blocks[columns[1, b]], weights[b * 3 + 1])
            acc += dot_nn(blocks[columns[2, b]], weights[b * 3 + 2])
            at = lane_block(b)
            store(at, joined(acc) + diagonal[:, at] * value[:, at])
        return carry

    lax.fori_loop(0, count // unroll, step, 0)


def own_blocks(blocks, value):
    own = value.shape[1] // TILE
    fill_blocks(blocks, value[...])
    zero = jnp.zeros(blocks.shape[1:], BF16)
    for i in range(own, blocks.shape[0]):
        blocks[i] = zero


def halo_products(place, spot, visits, weights, near, far, blocks):
    halos = blocks.shape[0]
    width = halos // 2
    fill_blocks(blocks.at[pl.ds(place[spot] * width, width)], near[...])
    fill_blocks(blocks.at[pl.ds((1 - place[spot]) * width, width)], far[...])
    found = []
    for i in range(2 * halos):
        acc = dot_nn(blocks[i % halos], weights[visits[2 * halos + i]])
        found.append((lane_block(visits[i]), joined(acc)))
    return found


def note_visits(columns, visits, own, halos):
    for i in range(2 * halos):
        visits[i] = 0
        visits[2 * halos + i] = 3 * own
    for b in range(own):
        for k in (1, 2):
            col = columns[k, b]

            @pl.when(col >= own)
            def _():
                at = (k - 1) * halos + col - own
                visits[at] = b
                visits[2 * halos + at] = 3 * b + k


def fetch(source, target, sems, chunks=CHUNKS):
    step = source.shape[0] // chunks
    copies = []
    for i in range(chunks):
        part = pl.ds(i * step, step)
        copies.append(pltpu.make_async_copy(source.at[part], target.at[part], sems.at[i]))
        copies[-1].start()
    return copies


def diagonal_scale(columns, tiles, scale, first, rows):
    lines = lax.broadcasted_iota(jnp.int32, (TILE, TILE), 0)
    lanes = lax.broadcasted_iota(jnp.int32, (TILE, TILE), 1)
    eye = lines == lanes

    def diagonal(b, k):
        return jnp.sum(jnp.where(eye, tiles[b, k], 0.0), axis=0, keepdims=True)

    for b in rows:
        here = slice(b * TILE, (b + 1) * TILE)
        mine = diagonal(b, 0)
        if first is not None:
            first[:, here] = mine
        scale[:, here] = mine
        for k in (1, 2):

            @pl.when(columns[k, b] == b)
            def _():
                scale[:, here] += diagonal(b, k)


def chunk_rows(i, count):
    step = count // CHUNKS
    return range(i * step, (i + 1) * step)


def pack_tile(tile):
    high, low = halves(tile.T)
    return jnp.concatenate([high, low], axis=0)


def pack_tiles(tiles, packed, which):
    rows = lax.broadcasted_iota(jnp.int32, (TILE, TILE), 0)
    lanes = lax.broadcasted_iota(jnp.int32, (TILE, TILE), 1)
    for b in which:
        packed[b * 3] = pack_tile(jnp.where(rows == lanes, 0.0, tiles[b, 0]))
        packed[b * 3 + 1] = pack_tile(tiles[b, 1])
        packed[b * 3 + 2] = pack_tile(tiles[b, 2])


def onehot_by_lane(index_row, rows):
    place = lax.broadcasted_iota(jnp.int32, (rows, index_row.shape[1]), 0)
    return jnp.where(place == index_row, 1.0, 0.0).astype(BF16)


def fill_picks(flag, sends, picks):
    up = flag == 1
    near = jnp.where(up, sends[1:2, :], sends[0:1, :])
    far = jnp.where(up, sends[0:1, :], sends[1:2, :])
    chosen = jnp.concatenate([near, far], axis=1)
    chunk = 256
    for i in range(picks.shape[0] // chunk):
        place = lax.broadcasted_iota(jnp.int32, (chunk, chosen.shape[1]), 0) + i * chunk
        picks[i * chunk : (i + 1) * chunk, :] = jnp.where(place == chosen, 1.0, 0.0).astype(BF16)


def put_pair(out, near, far):
    width = near.shape[1]
    near[...] = out[:, :width]
    far[...] = out[:, width:]


def pick_correction(out, part, picks, at):
    return out + joined(dot_nn(stacked(part), picks[at, :]))


def compact(wide, count):
    lanes = lax.broadcasted_iota(jnp.int32, (8, TILE), 1)
    sums = jnp.zeros((8, TILE), F32)
    for j in range(4):
        part = jnp.where(lanes < count, wide[8 * j : 8 * j + 8, :], 0.0)
        sums += pltpu.roll(part, count * j, 1) if j else part
    return sums


def spread_rows(sums, count):
    return jnp.concatenate(
        [sums] + [pltpu.roll(sums, TILE - count * j, 1) for j in range(1, 4)], axis=0
    )


def lane_columns(parts):
    lanes = lax.broadcasted_iota(jnp.int32, (32, TILE), 1)
    out = jnp.zeros((32, TILE), F32)
    for i, part in enumerate(parts):
        out = jnp.where(lanes == i, part, out)
    return out


def row_sum(value):
    return jnp.sum(value, axis=1, keepdims=True)


def copy_scalars(source, target):
    for k in range(source.shape[0]):
        for b in range(source.shape[1]):
            target[k, b] = source[k, b]


def first_kernel(
    place, columns, tiles_hbm, sends_hbm, source_hbm, *rest, lines,
):
    lines_hbm = rest[:lines]
    (scale, diagonal, start, near, far, picks, tiles, source, place_out, columns_out) = rest[
        lines : lines + 10
    ]
    kept = rest[lines + 10 : 2 * lines + 10]
    sends, sems = rest[2 * lines + 10 :]
    count = tiles.shape[0]
    early = pltpu.make_async_copy(sends_hbm, sends, sems.at[CHUNKS])
    early.start()
    copies = fetch(tiles_hbm, tiles, sems)
    others = [pltpu.make_async_copy(source_hbm, source, sems.at[CHUNKS + 1])]
    for i in range(lines):
        others.append(pltpu.make_async_copy(lines_hbm[i], kept[i], sems.at[CHUNKS + 2 + i]))
    for copy in others:
        copy.start()
    for i in range(place.shape[0]):
        place_out[i] = place[i]
    copy_scalars(columns, columns_out)
    early.wait()
    fill_picks(place[5], sends, picks)
    for i, copy in enumerate(copies):
        copy.wait()
        diagonal_scale(columns, tiles, scale, diagonal, chunk_rows(i, count))
    for copy in others:
        copy.wait()
    scale[...] = RELAXATION / scale[...]
    begin = scale[...] * source[...]
    start[...] = begin
    put_pair(select_nn(begin, picks[...]), near, far)


def pack_fine_kernel(columns, tiles, groups, packed, table, visits):
    own = tiles.shape[0]
    pack_tiles(tiles, packed, range(own))
    packed[3 * own] = jnp.zeros(packed.shape[1:], BF16)
    table[...] = onehot_by_lane(groups[...], table.shape[0])
    note_visits(columns, visits, own, 4)


def group_setup_kernel(
    place, columns, tiles_hbm, sends, weights, groups,
    scale, diagonal, packed, picks, table, raise_table, edge_near, edge_far, visits,
    columns_out, tiles, sems,
):
    count = tiles.shape[0]
    copies = fetch(tiles_hbm, tiles, sems)
    copy_scalars(columns, columns_out)
    note_visits(columns, visits, count, 2)
    fill_picks(place[6], sends, picks)
    table[...] = onehot_by_lane(groups[...], table.shape[0])
    raise_table[...] = onehot_by_lane(groups[...] + place[4], raise_table.shape[0])
    length = weights.shape[1]
    numbers = groups[...].astype(F32)
    lines = lax.broadcasted_iota(jnp.int32, (8, length), 0)
    facts = jnp.where(lines == 0, weights[...], jnp.where(lines == 1, numbers, 0.0))
    put_pair(select_nn(facts, picks[...]), edge_near, edge_far)
    for i, copy in enumerate(copies):
        copy.wait()
        diagonal_scale(columns, tiles, scale, diagonal, chunk_rows(i, count))
        pack_tiles(tiles, packed, chunk_rows(i, count))
    packed[3 * count] = jnp.zeros(packed.shape[1:], BF16)
    scale[...] = RELAXATION / scale[...]


def inner_restrict_kernel(
    columns, weights, diagonal, value, source, agg_weights, table, coarse, blocks, left
):
    own_blocks(blocks, value)

    def store(at, row):
        left[:, at] = (source[:, at] - row) * agg_weights[:, at]

    tile_rows(columns, weights, blocks, diagonal, value, store, value.shape[1] // TILE)
    coarse[...] = select_nt(left[...], table[...])


def restrict_kernel(
    place, visits, weights, coarse, far, near, agg_weights, table, *rest, spot, after
):
    lowered, blocks = rest[after:]
    out = coarse[...]
    for at, part in halo_products(place, spot, visits, weights, near, far, blocks):
        out -= joined(dot_nt(stacked(part * agg_weights[:, at]), table[:, at]))
    for i in range(lowered.shape[0]):
        lowered[i] = out


def group_start_kernel(gathered, scale, picks, *rest):
    facts = rest[:-4]
    group_rhs, start, near, far = rest[-4:]
    members = gathered.shape[0]
    width = group_rhs.shape[1] // members
    for i in range(members):
        group_rhs[:, i * width : (i + 1) * width] = gathered[i]
    begin = scale[...] * group_rhs[...]
    start[...] = begin
    rows = begin.shape[0]
    put_pair(select_nn(begin, picks[...]), near.at[:rows], far.at[:rows])
    if facts:
        near[rows:, :] = facts[0][...]
        far[rows:, :] = facts[1][...]


def coarse_setup_kernel(
    place, ccolumns, ctiles_hbm, after, cscale, cpacked, ccolumns_out, ctiles, cline, csems
):
    copies = fetch(ctiles_hbm, ctiles, csems)
    copy_scalars(ccolumns, ccolumns_out)
    blocks = ctiles.shape[0]
    for i, copy in enumerate(copies):
        copy.wait()
        diagonal_scale(ccolumns, ctiles, cline, None, chunk_rows(i, blocks))
    for b in range(blocks):
        cscale[b] = RELAXATION / cline[:, b * TILE : (b + 1) * TILE]
    for t in range(2):
        row = place[2 + t]
        for k in range(3):
            cpacked[t * 3 + k] = pack_tile(ctiles[row, k])


def group_restrict_kernel(
    place, visits, weights, coarse, far, near, agg_weights, table, *rest, edges
):
    rest = rest[1:] if edges else rest
    payload, blocks = rest[0], rest[-1]
    rows = coarse.shape[0]
    out = coarse[...]
    for at, part in halo_products(
        place, 6, visits, weights, near.at[:rows], far.at[:rows], blocks
    ):
        out -= joined(dot_nt(stacked(part * agg_weights[:, at]), table[:, at]))
    half = rows // 2
    message = jnp.concatenate([out[:half, :64], out[half:, :64]], axis=1)
    for i in range(payload.shape[0]):
        payload[i] = message
    if edges:
        edge_weights, edge_table = rest[1:3]
        base = place[4]
        up = place[6]
        low = jnp.where(up == 1, far[rows:, :], near[rows:, :])
        high = jnp.where(up == 1, near[rows:, :], far[rows:, :])
        edge_weights[...] = jnp.concatenate([low[0:1, :], high[0:1, :]], axis=1)
        numbers = jnp.concatenate(
            [
                low[1:2, :].astype(jnp.int32) + (base - 64),
                high[1:2, :].astype(jnp.int32) + (base + 64),
            ],
            axis=1,
        )
        edge_table[...] = onehot_by_lane(numbers, edge_table.shape[0])


def coarse_kernel(
    place, ccolumns, columns, gathered, cscale, cpacked, own_start, far, near,
    group_rhs, scale, diagonal, packed, group_weights, raise_table, edge_weights, edge_table,
    fine_start, fine_weights, fine_table, picks, fine_next, near_out, far_out, blocks, current,
):
    lanes = lax.broadcasted_iota(jnp.int32, (16, TILE), 1)

    def block(t):
        first = gathered[2 * t, :16, :]
        second = gathered[2 * t + 1, :16, :]
        top = jnp.where(lanes < 64, first, pltpu.roll(second, 64, 1))
        bottom = jnp.where(lanes < 64, pltpu.roll(first, 64, 1), second)
        return jnp.concatenate([top, bottom], axis=0)

    solved = []
    for t in range(2):
        row = place[2 + t]
        acc = jnp.zeros((64, TILE), F32)
        for k in range(3):
            col = ccolumns[k, row]
            acc += dot_nn(doubled(cscale[col] * block(col)), cpacked[t * 3 + k])
        mine = block(row)
        iterate = cscale[row] * mine
        solved.append(iterate + cscale[row] * (mine - joined(acc)))
    pair = jnp.concatenate(solved, axis=1)
    rows, length = own_start.shape
    half = near.shape[1]
    now = own_start[...] + select_nn(pair, raise_table[...]) * group_weights[...]
    raised = select_nn(pair, edge_table[...]) * edge_weights[...]
    current[...] = now
    fill_blocks(blocks, now)
    up = place[6]
    low = jnp.where(up == 1, far[:rows], near[:rows])
    high = jnp.where(up == 1, near[:rows], far[:rows])
    fill_blocks(blocks, low + raised[:, :half], length // TILE)
    fill_blocks(blocks, high + raised[:, half:], (length + half) // TILE)
    member = place[1]
    iterate_rows = []
    for j in range(2):
        b = member * 2 + j
        acc = dot_nn(blocks[columns[0, b]], packed[b * 3])
        acc += dot_nn(blocks[columns[1, b]], packed[b * 3 + 1])
        acc += dot_nn(blocks[columns[2, b]], packed[b * 3 + 2])
        at = lane_block(b)
        mine = current[:, at]
        image = joined(acc) + diagonal[:, at] * mine
        iterate_rows.append(mine + scale[:, at] * (group_rhs[:, at] - image))
    spread = jnp.concatenate(iterate_rows, axis=1)
    following = fine_start[...] + fine_weights[...] * select_nn(spread, fine_table[...])
    fine_next[...] = following
    put_pair(select_nn(following, picks[...]), near_out, far_out)


def inner_smooth_kernel(
    columns, weights, diagonal, value, source, scale, picks, smoothed, out, blocks
):
    own_blocks(blocks, value)

    def store(at, row):
        smoothed[:, at] = value[:, at] + scale[:, at] * (source[:, at] - row)

    tile_rows(columns, weights, blocks, diagonal, value, store, value.shape[1] // TILE)
    out[...] = select_nn(smoothed[...], picks[...])


def smooth_kernel(
    place, visits, weights, inner, inner_out, far, near, scale, picks,
    smoothed, near_out, far_out, blocks,
):
    smoothed[...] = inner[...]
    out = inner_out[...]
    for at, part in halo_products(place, 5, visits, weights, near, far, blocks):
        change = -scale[:, at] * part
        smoothed[:, at] += change
        out = pick_correction(out, change, picks, at)
    put_pair(out, near_out, far_out)


def inner_image_kernel(
    columns, weights, diagonal, value, scale, residual, picks, product, out, sums, blocks
):
    own_blocks(blocks, value)

    def store(at, row):
        product[:, at] = row

    tile_rows(columns, weights, blocks, diagonal, value, store, value.shape[1] // TILE)
    image = product[...]
    out[...] = select_nn(scale[...] * image, picks[...])
    field = value[...]
    sums[...] = lane_columns([row_sum(residual[...] * field), row_sum(field * image)])


def image_kernel(
    place, visits, weights, inner, inner_out, inner_sums, far, near, scale, value, picks,
    product, start, near_out, far_out, sums, blocks,
):
    product[...] = inner[...]
    out = inner_out[...]
    curve = jnp.zeros((32, TILE), F32)
    for at, part in halo_products(place, 5, visits, weights, near, far, blocks):
        product[:, at] += part
        curve += value[:, at] * part
        out = pick_correction(out, scale[:, at] * part, picks, at)
    put_pair(out, near_out, far_out)
    start[...] = scale[...] * product[...]
    sums[...] = inner_sums[...] + lane_columns([jnp.zeros((32, 1), F32), row_sum(curve)])


def inner_last_kernel(
    columns, weights, diagonal, second, residual, value, product, image, sums, blocks,
):
    own_blocks(blocks, second)

    def store(at, row):
        image[:, at] = row

    tile_rows(columns, weights, blocks, diagonal, second, store, second.shape[1] // TILE)
    follow = image[...]
    field = second[...]
    along = product[...]
    zero = jnp.zeros((32, 1), F32)
    sums[...] = lane_columns(
        [
            zero,
            zero,
            row_sum(residual[...] * field),
            row_sum(along * field),
            row_sum(value[...] * follow + field * along),
            row_sum(field * follow),
        ]
    )


def last_kernel(
    place, visits, weights, inner, inner_sums, first_sums, far, near, value, second,
    image, copies, blocks,
):
    image[...] = inner[...]
    cross = jnp.zeros((32, TILE), F32)
    curve = jnp.zeros((32, TILE), F32)
    for at, part in halo_products(place, 5, visits, weights, near, far, blocks):
        image[:, at] += part
        cross += value[:, at] * part
        curve += second[:, at] * part
    zero = jnp.zeros((32, 1), F32)
    sums = inner_sums[...] + first_sums[...]
    sums += lane_columns([zero, zero, zero, zero, row_sum(cross), row_sum(curve)])
    message = compact(sums, 6)
    for i in range(copies.shape[0]):
        copies[i] = message


def sum_copies_kernel(parts, copies):
    total = parts[0]
    for i in range(1, parts.shape[0]):
        total += parts[i]
    for i in range(copies.shape[0]):
        copies[i] = total


def final_kernel(parts, start, value, product, second, image, solution, residual):
    small = parts[0]
    for i in range(1, parts.shape[0]):
        small += parts[i]
    sums = spread_rows(small, 6)
    energy, curve, along, across, cross, last = (sums[:, i : i + 1] for i in range(6))
    step = energy / curve
    new = step * (step * across - along)
    ratio = new / energy
    grown = 1.0 + ratio
    second_curve = grown * (grown * curve - step * cross) + step * step * last
    second_step = new / second_curve
    field = value[...]
    product_now = product[...]
    solution[...] = step * field + second_step * (grown * field - step * second[...])
    residual[...] = (start[...] - step * product_now) - second_step * (
        grown * product_now - step * image[...]
    )


def neighbours(near_out, far_out, axes):
    count = lax.axis_size(axes)
    near = [(i, i ^ 1) for i in range(count)]
    far = [(i, i + 1) for i in range(1, count - 1, 2)]
    far = far + [(b, a) for a, b in far]
    far_in = lax.ppermute(far_out, axes, far)
    return lax.ppermute(near_out, axes, near), far_in


def exchanged(copies, axes):
    return lax.all_to_all(copies, axes, split_axis=0, concat_axis=0, tiled=True)


def shards(
    right_side,
    fine_tiles,
    fine_columns,
    fine_sends,
    fine_weights,
    fine_groups,
    group_tiles,
    group_columns,
    group_sends,
    group_weights,
    group_groups,
    coarse_tiles,
    coarse_columns,
):
    rhs, length = right_side.shape
    fine_count = length // AGG1
    group_length = group_weights.shape[0]
    share = group_length // AGG2
    members = lax.axis_size(MEM)
    group_total = lax.axis_size(GRP)
    fine_half = fine_sends.shape[1]
    group_half = group_sends.shape[1]
    fine_halo = 2 * fine_half // TILE
    group_halo = 2 * group_half // TILE
    fine_blocks = length // TILE
    group_blocks = group_length // TILE
    coarse_blocks = coarse_tiles.shape[0]

    fine_weights = fine_weights.reshape(1, -1)
    fine_groups = fine_groups.reshape(1, -1)
    group_weights = group_weights.reshape(1, -1)
    group_groups = group_groups.reshape(1, -1)
    fine_columns = fine_columns.T
    group_columns = group_columns.T
    coarse_columns = coarse_columns.T

    grp = lax.axis_index(GRP)
    mem = lax.axis_index(MEM)
    row_a = jnp.maximum((grp - 1) // 2, 0)
    row_b = jnp.minimum(row_a + 1, coarse_blocks - 1)
    place = jnp.stack(
        [grp, mem, row_a, row_b, grp * share - row_a * TILE, 1 - mem % 2, 1 - grp % 2]
    ).astype(jnp.int32)

    def block_scratch(count):
        return pltpu.VMEM((count, 2 * rhs, 2 * TILE), BF16)

    edge = shape((rhs, fine_half))
    group_edge = shape((rhs, group_half))
    field = shape((rhs, length))
    line = shape((1, length))
    small = shape((rhs, TILE))
    picked = shape((rhs, 2 * fine_half))

    pinned = [
        pltpu.with_memory_space_constraint(x, pltpu.HBM)
        for x in (fine_tiles, fine_sends, right_side, fine_weights, fine_groups, group_weights,
                  group_groups, group_sends)
    ]
    group_tiles = pltpu.with_memory_space_constraint(group_tiles, pltpu.HBM)
    coarse_tiles = pltpu.with_memory_space_constraint(coarse_tiles, pltpu.HBM)
    (fine_scale, fine_diagonal, fine_start, near, far, fine_picks, fine_tiles, right_side,
     place, fine_columns, fine_weights, fine_groups, group_weights, group_groups,
     group_sends) = run(
        functools.partial(first_kernel, lines=5), "first",
        [line, line, field, edge, edge, shape((length, 2 * fine_half), BF16),
         shape(fine_tiles.shape), field, scalars(7), pltpu.SMEM(fine_columns.shape, jnp.int32),
         line, shape((1, length), jnp.int32), line, shape((1, group_length), jnp.int32),
         shape(group_sends.shape, jnp.int32)],
        [place, fine_columns] + pinned, smem=(0, 1), hbm_args=range(2, 10), smem_outs=(8, 9),
        scratch=[pltpu.VMEM(fine_sends.shape, jnp.int32),
                 pltpu.SemaphoreType.DMA((CHUNKS + 7,))],
    )
    near, far = neighbours(near, far, ALL)
    fine_packed, fine_table, fine_visits = run(
        pack_fine_kernel, "pack_fine",
        [shape((3 * fine_blocks + 1, 2 * TILE, TILE), BF16), shape((fine_count, length), BF16),
         scalars(4 * fine_halo)],
        (fine_columns, fine_tiles, fine_groups), smem=(0,), smem_outs=(2,),
    )

    (group_scale, group_diagonal, group_packed, group_picks, group_table, raise_table,
     edge_near, edge_far, group_visits, group_columns) = run(
        group_setup_kernel, "group_setup",
        [
            line,
            line,
            shape((3 * group_blocks + 1, 2 * TILE, TILE), BF16),
            shape((group_length, 2 * group_half), BF16),
            shape((TILE, group_length), BF16),
            shape((2 * TILE, group_length), BF16),
            shape((8, group_half)),
            shape((8, group_half)),
            scalars(4 * group_halo),
            pltpu.SMEM(group_columns.shape, jnp.int32),
        ],
        (place, group_columns, group_tiles, group_sends, group_weights, group_groups),
        smem=(0, 1), smem_outs=(8, 9), hbm_args=(2,),
        scratch=[pltpu.VMEM(group_tiles.shape, F32), pltpu.SemaphoreType.DMA((CHUNKS,))],
    )
    facts = (edge_near, edge_far)
    def coarse_parts(after):
        return run(
            coarse_setup_kernel, "coarse_setup",
            [
                shape((coarse_blocks, 1, TILE)),
                shape((6, 2 * TILE, TILE), BF16),
                pltpu.SMEM(coarse_columns.shape, jnp.int32),
            ],
            (place, coarse_columns, coarse_tiles, after), smem=(0, 1), smem_outs=(2,),
            hbm_args=(2,),
            scratch=[pltpu.VMEM(coarse_tiles.shape, F32),
                     pltpu.VMEM((1, coarse_blocks * TILE), F32),
                     pltpu.SemaphoreType.DMA((CHUNKS,))],
        )

    kept = {}

    def vcycle(source, fine_start, near, far, edges, held):
        coarse = run(
            inner_restrict_kernel, "inner_restrict", [shape((rhs, fine_count))],
            (fine_columns, fine_packed, fine_diagonal, fine_start, source, fine_weights,
             fine_table),
            smem=(0,), scratch=[block_scratch(fine_blocks + fine_halo), pltpu.VMEM((rhs, length), F32)],
        )[0]
        lowered = run(
            functools.partial(restrict_kernel, spot=5, after=len(held)), "restrict",
            [shape((members, rhs, fine_count))],
            (place, fine_visits, fine_packed, coarse, far, near, fine_weights, fine_table)
            + held,
            smem=(0, 1), scratch=[block_scratch(fine_halo)],
        )[0]
        gathered = exchanged(lowered, MEM)
        extra = facts if edges is None else ()
        message = shape((rhs + 8 * bool(extra), group_half))
        group_rhs, group_start, near, far = run(
            group_start_kernel, "group_start", [field, field, message, message],
            (gathered, group_scale, group_picks) + extra,
        )
        g_near, g_far = neighbours(near, far, GRP)
        if edges is None:
            kept["coarse"] = coarse_parts(near)
        coarse_scale, coarse_packed, coarse_cols = kept["coarse"]
        coarse = run(
            inner_restrict_kernel, "group_inner", [shape((rhs, TILE))],
            (group_columns, group_packed, group_diagonal, group_start, group_rhs,
             group_weights, group_table),
            smem=(0,), scratch=[block_scratch(group_blocks + group_halo), pltpu.VMEM((rhs, length), F32)],
        )[0]
        payload, *made = run(
            functools.partial(group_restrict_kernel, edges=edges is None), "group_restrict",
            [shape((group_total, 16, TILE))]
            + ([shape((1, 2 * group_half)), shape((2 * TILE, 2 * group_half), BF16)]
               if edges is None else []),
            (place, group_visits, group_packed, coarse, g_far, g_near, group_weights,
             group_table) + ((coarse_scale,) if edges is None else ()),
            smem=(0, 1), scratch=[block_scratch(group_halo)],
        )
        edges = tuple(made) if edges is None else edges
        gathered = exchanged(payload, GRP)
        fine_next, near, far = run(
            coarse_kernel, "coarse", [field, edge, edge],
            (place, coarse_cols, group_columns, gathered, coarse_scale, coarse_packed,
             group_start, g_far, g_near, group_rhs, group_scale, group_diagonal, group_packed,
             group_weights, raise_table, *edges, fine_start, fine_weights, fine_table,
             fine_picks),
            smem=(0, 1, 2),
            scratch=[block_scratch(group_blocks + group_halo), pltpu.VMEM((rhs, length), F32)],
        )
        near, far = neighbours(near, far, ALL)
        inside, out = run(
            inner_smooth_kernel, "inner_smooth", [field, picked],
            (fine_columns, fine_packed, fine_diagonal, fine_next, source, fine_scale,
             fine_picks),
            smem=(0,), scratch=[block_scratch(fine_blocks + fine_halo)],
        )
        smoothed, near, far = run(
            smooth_kernel, "smooth", [field, edge, edge],
            (place, fine_visits, fine_packed, inside, out, far, near, fine_scale, fine_picks),
            smem=(0, 1), scratch=[block_scratch(fine_halo)],
        )
        near, far = neighbours(near, far, ALL)
        return smoothed, near, far, edges

    value, near, far, edges = vcycle(right_side, fine_start, near, far, None, (edge_near,))
    inside, out, sums = run(
        inner_image_kernel, "inner_image", [field, picked, small],
        (fine_columns, fine_packed, fine_diagonal, value, fine_scale, right_side, fine_picks),
        smem=(0,), scratch=[block_scratch(fine_blocks + fine_halo)],
    )
    product, start, near, far, sums = run(
        image_kernel, "image", [field, field, edge, edge, small],
        (place, fine_visits, fine_packed, inside, out, sums, far, near, fine_scale, value,
         fine_picks),
        smem=(0, 1), scratch=[block_scratch(fine_halo)],
    )
    near, far = neighbours(near, far, ALL)
    second, near, far, _ = vcycle(product, start, near, far, edges, ())
    inside, more = run(
        inner_last_kernel, "inner_last", [field, small],
        (fine_columns, fine_packed, fine_diagonal, second, right_side, value, product),
        smem=(0,), scratch=[block_scratch(fine_blocks + fine_halo)],
    )
    image, copies = run(
        last_kernel, "last", [field, shape((members, 8, TILE))],
        (place, fine_visits, fine_packed, inside, more, sums, far, near, value, second),
        smem=(0, 1), scratch=[block_scratch(fine_halo)],
    )
    copies = run(
        sum_copies_kernel, "sum_copies", [shape((group_total, 8, TILE))],
        (exchanged(copies, MEM),),
    )[0]
    parts = exchanged(copies, GRP)
    solution, residual = run(
        final_kernel, "final", [hbm((rhs, length)), hbm((rhs, length))],
        (parts, right_side, value, product, second, image),
    )
    return solution, residual


def solution(mesh):
    finer = Mesh(mesh.devices.reshape(8, 4, 4, 2), ALL)
    return jax.shard_map(
        shards,
        mesh=finer,
        in_specs=(
            P(None, ALL),
            P(ALL, None, None, None),
            P(ALL, None),
            P(ALL, None),
            P(ALL),
            P(ALL),
            P(GRP, None, None, None),
            P(GRP, None),
            P(GRP, None),
            P(GRP),
            P(GRP),
            P(),
            P(),
        ),
        out_specs=(P(None, ALL), P(None, ALL)),
        check_vma=False,
    )
```

```python
import functools

import jax
import jax.numpy as jnp
from jax import lax
from jax.experimental import pallas as pl
from jax.experimental.pallas import tpu as pltpu
from jax.sharding import Mesh
from jax.sharding import PartitionSpec as P

TILE = 128
AGG1 = 8
AGG2 = 32
ALL = ("grp_0", "grp_1", "mem_0", "mem_1")
GRP = ("grp_0", "grp_1")
MEM = ("mem_0", "mem_1")
RELAXATION = 0.7
F32 = jnp.float32
BF16 = jnp.bfloat16
VMEM_SPEC = pl.BlockSpec(memory_space=pltpu.VMEM)
SMEM_SPEC = pl.BlockSpec(memory_space=pltpu.SMEM)
HBM_SPEC = pl.BlockSpec(memory_space=pltpu.HBM)
CHUNKS = 8
LIMIT = 24 * 1024 * 1024


def shape(dims, dtype=F32):
    return pltpu.VMEM(tuple(dims), dtype)


def hbm(dims, dtype=F32):
    return jax.ShapeDtypeStruct(tuple(dims), dtype)


def scalars(count):
    return pltpu.SMEM((count,), jnp.int32)


def run(
    kernel, name, outs, args, smem=(), hbm_args=(), scratch=(), smem_outs=(), flops=4_000_000_000
):
    specs = [
        SMEM_SPEC if i in smem else HBM_SPEC if i in hbm_args else VMEM_SPEC
        for i in range(len(args))
    ]
    return pl.pallas_call(
        kernel,
        name=name,
        out_shape=tuple(outs),
        in_specs=specs,
        out_specs=tuple(SMEM_SPEC if i in smem_outs else VMEM_SPEC for i in range(len(outs))),
        scratch_shapes=list(scratch),
        compiler_params=pltpu.CompilerParams(vmem_limit_bytes=LIMIT),
        cost_estimate=pl.CostEstimate(flops=flops, transcendentals=0, bytes_accessed=4_000_000),
    )(*args)


def halves(value):
    high = value.astype(BF16)
    low = (value - high.astype(F32)).astype(BF16)
    return high, low


def stacked(value):
    high, low = halves(value)
    return jnp.concatenate([high, low], axis=0)


def doubled(value):
    both = stacked(value)
    return jnp.concatenate([both, both], axis=1)


def joined(both):
    rows = both.shape[0] // 2
    return both[:rows] + both[rows:]


def dot_nt(left, right):
    return lax.dot_general(left, right, (((1,), (1,)), ((), ())), preferred_element_type=F32)


def dot_nn(left, right):
    return lax.dot_general(left, right, (((1,), (0,)), ((), ())), preferred_element_type=F32)


def select_nn(value, onehot):
    return joined(dot_nn(stacked(value), onehot))


def select_nt(value, onehot):
    return joined(dot_nt(stacked(value), onehot))


def fill_blocks(blocks, value, first=0):
    for i in range(value.shape[1] // TILE):
        blocks[first + i] = doubled(value[:, i * TILE : (i + 1) * TILE])


def lane_block(b):
    return pl.ds(pl.multiple_of(b * TILE, TILE), TILE)


def tile_rows(columns, weights, blocks, diagonal, value, store, count, unroll=4):
    def step(i, carry):
        for j in range(unroll):
            b = i * unroll + j
            acc = dot_nn(blocks[columns[0, b]], weights[b * 3])
            acc += dot_nn(blocks[columns[1, b]], weights[b * 3 + 1])
            acc += dot_nn(blocks[columns[2, b]], weights[b * 3 + 2])
            at = lane_block(b)
            store(at, joined(acc) + diagonal[:, at] * value[:, at])
        return carry

    lax.fori_loop(0, count // unroll, step, 0)


def own_blocks(blocks, value):
    own = value.shape[1] // TILE
    fill_blocks(blocks, value[...])
    zero = jnp.zeros(blocks.shape[1:], BF16)
    for i in range(own, blocks.shape[0]):
        blocks[i] = zero


def halo_products(place, spot, visits, weights, near, far, blocks):
    halos = blocks.shape[0]
    width = halos // 2
    fill_blocks(blocks.at[pl.ds(place[spot] * width, width)], near[...])
    fill_blocks(blocks.at[pl.ds((1 - place[spot]) * width, width)], far[...])
    found = []
    for i in range(2 * halos):
        acc = dot_nn(blocks[i % halos], weights[visits[2 * halos + i]])
        found.append((lane_block(visits[i]), joined(acc)))
    return found


def note_visits(columns, visits, own, halos):
    for i in range(2 * halos):
        visits[i] = 0
        visits[2 * halos + i] = 3 * own
    for b in range(own):
        for k in (1, 2):
            col = columns[k, b]

            @pl.when(col >= own)
            def _():
                at = (k - 1) * halos + col - own
                visits[at] = b
                visits[2 * halos + at] = 3 * b + k


def fetch(source, target, sems, chunks=CHUNKS):
    step = source.shape[0] // chunks
    copies = []
    for i in range(chunks):
        part = pl.ds(i * step, step)
        copies.append(pltpu.make_async_copy(source.at[part], target.at[part], sems.at[i]))
        copies[-1].start()
    return copies


def diagonal_scale(columns, tiles, scale, first, rows):
    lines = lax.broadcasted_iota(jnp.int32, (TILE, TILE), 0)
    lanes = lax.broadcasted_iota(jnp.int32, (TILE, TILE), 1)
    eye = lines == lanes

    def diagonal(b, k):
        return jnp.sum(jnp.where(eye, tiles[b, k], 0.0), axis=0, keepdims=True)

    for b in rows:
        here = slice(b * TILE, (b + 1) * TILE)
        mine = diagonal(b, 0)
        if first is not None:
            first[:, here] = mine
        scale[:, here] = mine
        for k in (1, 2):

            @pl.when(columns[k, b] == b)
            def _():
                scale[:, here] += diagonal(b, k)


def chunk_rows(i, count):
    step = count // CHUNKS
    return range(i * step, (i + 1) * step)


def pack_tile(tile):
    high, low = halves(tile.T)
    return jnp.concatenate([high, low], axis=0)


def pack_tiles(tiles, packed, which):
    rows = lax.broadcasted_iota(jnp.int32, (TILE, TILE), 0)
    lanes = lax.broadcasted_iota(jnp.int32, (TILE, TILE), 1)
    for b in which:
        packed[b * 3] = pack_tile(jnp.where(rows == lanes, 0.0, tiles[b, 0]))
        packed[b * 3 + 1] = pack_tile(tiles[b, 1])
        packed[b * 3 + 2] = pack_tile(tiles[b, 2])


def onehot_by_lane(index_row, rows):
    place = lax.broadcasted_iota(jnp.int32, (rows, index_row.shape[1]), 0)
    return jnp.where(place == index_row, 1.0, 0.0).astype(BF16)


def fill_picks(flag, sends, picks):
    up = flag == 1
    near = jnp.where(up, sends[1:2, :], sends[0:1, :])
    far = jnp.where(up, sends[0:1, :], sends[1:2, :])
    chosen = jnp.concatenate([near, far], axis=1)
    chunk = 256
    for i in range(picks.shape[0] // chunk):
        place = lax.broadcasted_iota(jnp.int32, (chunk, chosen.shape[1]), 0) + i * chunk
        picks[i * chunk : (i + 1) * chunk, :] = jnp.where(place == chosen, 1.0, 0.0).astype(BF16)


def put_pair(out, near, far):
    width = near.shape[1]
    near[...] = out[:, :width]
    far[...] = out[:, width:]


def pick_correction(out, part, picks, at):
    return out + joined(dot_nn(stacked(part), picks[at, :]))


def compact(wide, count):
    lanes = lax.broadcasted_iota(jnp.int32, (8, TILE), 1)
    sums = jnp.zeros((8, TILE), F32)
    for j in range(4):
        part = jnp.where(lanes < count, wide[8 * j : 8 * j + 8, :], 0.0)
        sums += pltpu.roll(part, count * j, 1) if j else part
    return sums


def spread_rows(sums, count):
    return jnp.concatenate(
        [sums] + [pltpu.roll(sums, TILE - count * j, 1) for j in range(1, 4)], axis=0
    )


def lane_columns(parts):
    lanes = lax.broadcasted_iota(jnp.int32, (32, TILE), 1)
    out = jnp.zeros((32, TILE), F32)
    for i, part in enumerate(parts):
        out = jnp.where(lanes == i, part, out)
    return out


def row_sum(value):
    return jnp.sum(value, axis=1, keepdims=True)


def copy_scalars(source, target):
    for k in range(source.shape[0]):
        for b in range(source.shape[1]):
            target[k, b] = source[k, b]


def first_kernel(
    place, columns, tiles_hbm, sends_hbm, source_hbm, *rest, lines,
):
    lines_hbm = rest[:lines]
    (scale, diagonal, start, near, far, picks, tiles, source, place_out, columns_out) = rest[
        lines : lines + 10
    ]
    kept = rest[lines + 10 : 2 * lines + 10]
    sends, sems = rest[2 * lines + 10 :]
    count = tiles.shape[0]
    early = pltpu.make_async_copy(sends_hbm, sends, sems.at[CHUNKS])
    early.start()
    copies = fetch(tiles_hbm, tiles, sems)
    others = [pltpu.make_async_copy(source_hbm, source, sems.at[CHUNKS + 1])]
    for i in range(lines):
        others.append(pltpu.make_async_copy(lines_hbm[i], kept[i], sems.at[CHUNKS + 2 + i]))
    for copy in others:
        copy.start()
    for i in range(place.shape[0]):
        place_out[i] = place[i]
    copy_scalars(columns, columns_out)
    early.wait()
    fill_picks(place[5], sends, picks)
    for i, copy in enumerate(copies):
        copy.wait()
        diagonal_scale(columns, tiles, scale, diagonal, chunk_rows(i, count))
    for copy in others:
        copy.wait()
    scale[...] = RELAXATION / scale[...]
    begin = scale[...] * source[...]
    start[...] = begin
    put_pair(select_nn(begin, picks[...]), near, far)


def pack_fine_kernel(columns, tiles, groups, packed, table, visits):
    own = tiles.shape[0]
    pack_tiles(tiles, packed, range(own))
    packed[3 * own] = jnp.zeros(packed.shape[1:], BF16)
    table[...] = onehot_by_lane(groups[...], table.shape[0])
    note_visits(columns, visits, own, 4)


def group_setup_kernel(
    place, columns, tiles_hbm, sends, weights, groups,
    scale, diagonal, tiles, picks, edge_near, edge_far, visits, columns_out, sems,
):
    count = tiles.shape[0]
    copies = fetch(tiles_hbm, tiles, sems)
    copy_scalars(columns, columns_out)
    note_visits(columns, visits, count, 2)
    fill_picks(place[6], sends, picks)
    length = weights.shape[1]
    numbers = groups[...].astype(F32)
    lines = lax.broadcasted_iota(jnp.int32, (8, length), 0)
    facts = jnp.where(lines == 0, weights[...], jnp.where(lines == 1, numbers, 0.0))
    put_pair(select_nn(facts, picks[...]), edge_near, edge_far)
    for i, copy in enumerate(copies):
        copy.wait()
        diagonal_scale(columns, tiles, scale, diagonal, chunk_rows(i, count))
    scale[...] = RELAXATION / scale[...]


def group_pack_kernel(tiles, after, packed):
    count = tiles.shape[0]
    pack_tiles(tiles, packed, range(count))
    packed[3 * count] = jnp.zeros(packed.shape[1:], BF16)


def inner_restrict_kernel(
    columns, weights, diagonal, value, source, agg_weights, table, coarse, blocks, left
):
    own_blocks(blocks, value)

    def store(at, row):
        left[:, at] = (source[:, at] - row) * agg_weights[:, at]

    tile_rows(columns, weights, blocks, diagonal, value, store, value.shape[1] // TILE)
    coarse[...] = select_nt(left[...], table[...])


def restrict_kernel(
    place, visits, weights, coarse, far, near, agg_weights, table, *rest, spot, after
):
    lowered, blocks = rest[after:]
    out = coarse[...]
    for at, part in halo_products(place, spot, visits, weights, near, far, blocks):
        out -= joined(dot_nt(stacked(part * agg_weights[:, at]), table[:, at]))
    for i in range(lowered.shape[0]):
        lowered[i] = out


def group_start_kernel(gathered, scale, picks, *rest):
    facts = rest[:-4]
    group_rhs, start, near, far = rest[-4:]
    members = gathered.shape[0]
    width = group_rhs.shape[1] // members
    for i in range(members):
        group_rhs[:, i * width : (i + 1) * width] = gathered[i]
    begin = scale[...] * group_rhs[...]
    start[...] = begin
    rows = begin.shape[0]
    put_pair(select_nn(begin, picks[...]), near.at[:rows], far.at[:rows])
    if facts:
        near[rows:, :] = facts[0][...]
        far[rows:, :] = facts[1][...]


def coarse_setup_kernel(
    place, ccolumns, ctiles_hbm, groups, after, cscale, cpacked, ccolumns_out, table, raise_table,
    ctiles, cline, csems,
):
    copies = fetch(ctiles_hbm, ctiles, csems)
    copy_scalars(ccolumns, ccolumns_out)
    table[...] = onehot_by_lane(groups[...], table.shape[0])
    raise_table[...] = onehot_by_lane(groups[...] + place[4], raise_table.shape[0])
    blocks = ctiles.shape[0]
    for i, copy in enumerate(copies):
        copy.wait()
        diagonal_scale(ccolumns, ctiles, cline, None, chunk_rows(i, blocks))
    for b in range(blocks):
        cscale[b] = RELAXATION / cline[:, b * TILE : (b + 1) * TILE]
    for t in range(2):
        row = place[2 + t]
        for k in range(3):
            cpacked[t * 3 + k] = pack_tile(ctiles[row, k])


def group_restrict_kernel(
    place, visits, weights, coarse, far, near, agg_weights, table, *rest, edges
):
    rest = rest[1:] if edges else rest
    payload, blocks = rest[0], rest[-1]
    rows = coarse.shape[0]
    out = coarse[...]
    for at, part in halo_products(
        place, 6, visits, weights, near.at[:rows], far.at[:rows], blocks
    ):
        out -= joined(dot_nt(stacked(part * agg_weights[:, at]), table[:, at]))
    half = rows // 2
    message = jnp.concatenate([out[:half, :64], out[half:, :64]], axis=1)
    for i in range(payload.shape[0]):
        payload[i] = message
    if edges:
        edge_weights, edge_table = rest[1:3]
        base = place[4]
        up = place[6]
        low = jnp.where(up == 1, far[rows:, :], near[rows:, :])
        high = jnp.where(up == 1, near[rows:, :], far[rows:, :])
        edge_weights[...] = jnp.concatenate([low[0:1, :], high[0:1, :]], axis=1)
        numbers = jnp.concatenate(
            [
                low[1:2, :].astype(jnp.int32) + (base - 64),
                high[1:2, :].astype(jnp.int32) + (base + 64),
            ],
            axis=1,
        )
        edge_table[...] = onehot_by_lane(numbers, edge_table.shape[0])


def coarse_kernel(
    place, ccolumns, columns, gathered, cscale, cpacked, own_start, far, near,
    group_rhs, scale, diagonal, packed, group_weights, raise_table, edge_weights, edge_table,
    fine_start, fine_weights, fine_table, picks, fine_next, near_out, far_out, blocks, current,
):
    lanes = lax.broadcasted_iota(jnp.int32, (16, TILE), 1)

    def block(t):
        first = gathered[2 * t, :16, :]
        second = gathered[2 * t + 1, :16, :]
        top = jnp.where(lanes < 64, first, pltpu.roll(second, 64, 1))
        bottom = jnp.where(lanes < 64, pltpu.roll(first, 64, 1), second)
        return jnp.concatenate([top, bottom], axis=0)

    solved = []
    for t in range(2):
        row = place[2 + t]
        acc = jnp.zeros((64, TILE), F32)
        for k in range(3):
            col = ccolumns[k, row]
            acc += dot_nn(doubled(cscale[col] * block(col)), cpacked[t * 3 + k])
        mine = block(row)
        iterate = cscale[row] * mine
        solved.append(iterate + cscale[row] * (mine - joined(acc)))
    pair = jnp.concatenate(solved, axis=1)
    rows, length = own_start.shape
    half = near.shape[1]
    now = own_start[...] + select_nn(pair, raise_table[...]) * group_weights[...]
    raised = select_nn(pair, edge_table[...]) * edge_weights[...]
    current[...] = now
    fill_blocks(blocks, now)
    up = place[6]
    low = jnp.where(up == 1, far[:rows], near[:rows])
    high = jnp.where(up == 1, near[:rows], far[:rows])
    fill_blocks(blocks, low + raised[:, :half], length // TILE)
    fill_blocks(blocks, high + raised[:, half:], (length + half) // TILE)
    member = place[1]
    iterate_rows = []
    for j in range(2):
        b = member * 2 + j
        acc = dot_nn(blocks[columns[0, b]], packed[b * 3])
        acc += dot_nn(blocks[columns[1, b]], packed[b * 3 + 1])
        acc += dot_nn(blocks[columns[2, b]], packed[b * 3 + 2])
        at = lane_block(b)
        mine = current[:, at]
        image = joined(acc) + diagonal[:, at] * mine
        iterate_rows.append(mine + scale[:, at] * (group_rhs[:, at] - image))
    spread = jnp.concatenate(iterate_rows, axis=1)
    following = fine_start[...] + fine_weights[...] * select_nn(spread, fine_table[...])
    fine_next[...] = following
    put_pair(select_nn(following, picks[...]), near_out, far_out)


def inner_smooth_kernel(
    columns, weights, diagonal, value, source, scale, picks, smoothed, out, blocks
):
    own_blocks(blocks, value)

    def store(at, row):
        smoothed[:, at] = value[:, at] + scale[:, at] * (source[:, at] - row)

    tile_rows(columns, weights, blocks, diagonal, value, store, value.shape[1] // TILE)
    out[...] = select_nn(smoothed[...], picks[...])


def smooth_kernel(
    place, visits, weights, inner, inner_out, far, near, scale, picks,
    smoothed, near_out, far_out, blocks,
):
    smoothed[...] = inner[...]
    out = inner_out[...]
    for at, part in halo_products(place, 5, visits, weights, near, far, blocks):
        change = -scale[:, at] * part
        smoothed[:, at] += change
        out = pick_correction(out, change, picks, at)
    put_pair(out, near_out, far_out)


def inner_image_kernel(
    columns, weights, diagonal, value, scale, residual, picks, product, out, sums, blocks
):
    own_blocks(blocks, value)

    def store(at, row):
        product[:, at] = row

    tile_rows(columns, weights, blocks, diagonal, value, store, value.shape[1] // TILE)
    image = product[...]
    out[...] = select_nn(scale[...] * image, picks[...])
    field = value[...]
    sums[...] = lane_columns([row_sum(residual[...] * field), row_sum(field * image)])


def image_kernel(
    place, visits, weights, inner, inner_out, inner_sums, far, near, scale, value, picks,
    product, start, near_out, far_out, sums, blocks,
):
    product[...] = inner[...]
    out = inner_out[...]
    curve = jnp.zeros((32, TILE), F32)
    for at, part in halo_products(place, 5, visits, weights, near, far, blocks):
        product[:, at] += part
        curve += value[:, at] * part
        out = pick_correction(out, scale[:, at] * part, picks, at)
    put_pair(out, near_out, far_out)
    start[...] = scale[...] * product[...]
    sums[...] = inner_sums[...] + lane_columns([jnp.zeros((32, 1), F32), row_sum(curve)])


def inner_last_kernel(
    columns, weights, diagonal, second, residual, value, product, image, sums, blocks,
):
    own_blocks(blocks, second)

    def store(at, row):
        image[:, at] = row

    tile_rows(columns, weights, blocks, diagonal, second, store, second.shape[1] // TILE)
    follow = image[...]
    field = second[...]
    along = product[...]
    zero = jnp.zeros((32, 1), F32)
    sums[...] = lane_columns(
        [
            zero,
            zero,
            row_sum(residual[...] * field),
            row_sum(along * field),
            row_sum(value[...] * follow + field * along),
            row_sum(field * follow),
        ]
    )


def last_kernel(
    place, visits, weights, inner, inner_sums, first_sums, far, near, value, second,
    image, copies, blocks,
):
    image[...] = inner[...]
    cross = jnp.zeros((32, TILE), F32)
    curve = jnp.zeros((32, TILE), F32)
    for at, part in halo_products(place, 5, visits, weights, near, far, blocks):
        image[:, at] += part
        cross += value[:, at] * part
        curve += second[:, at] * part
    zero = jnp.zeros((32, 1), F32)
    sums = inner_sums[...] + first_sums[...]
    sums += lane_columns([zero, zero, zero, zero, row_sum(cross), row_sum(curve)])
    message = compact(sums, 6)
    for i in range(copies.shape[0]):
        copies[i] = message


def sum_copies_kernel(parts, copies):
    total = parts[0]
    for i in range(1, parts.shape[0]):
        total += parts[i]
    for i in range(copies.shape[0]):
        copies[i] = total


def final_kernel(parts, start, value, product, second, image, solution, residual):
    small = parts[0]
    for i in range(1, parts.shape[0]):
        small += parts[i]
    sums = spread_rows(small, 6)
    energy, curve, along, across, cross, last = (sums[:, i : i + 1] for i in range(6))
    step = energy / curve
    new = step * (step * across - along)
    ratio = new / energy
    grown = 1.0 + ratio
    second_curve = grown * (grown * curve - step * cross) + step * step * last
    second_step = new / second_curve
    field = value[...]
    product_now = product[...]
    solution[...] = step * field + second_step * (grown * field - step * second[...])
    residual[...] = (start[...] - step * product_now) - second_step * (
        grown * product_now - step * image[...]
    )


def neighbours(near_out, far_out, axes):
    count = lax.axis_size(axes)
    near = [(i, i ^ 1) for i in range(count)]
    far = [(i, i + 1) for i in range(1, count - 1, 2)]
    far = far + [(b, a) for a, b in far]
    far_in = lax.ppermute(far_out, axes, far)
    return lax.ppermute(near_out, axes, near), far_in


def exchanged(copies, axes):
    return lax.all_to_all(copies, axes, split_axis=0, concat_axis=0, tiled=True)


def shards(
    right_side,
    fine_tiles,
    fine_columns,
    fine_sends,
    fine_weights,
    fine_groups,
    group_tiles,
    group_columns,
    group_sends,
    group_weights,
    group_groups,
    coarse_tiles,
    coarse_columns,
):
    rhs, length = right_side.shape
    fine_count = length // AGG1
    group_length = group_weights.shape[0]
    share = group_length // AGG2
    members = lax.axis_size(MEM)
    group_total = lax.axis_size(GRP)
    fine_half = fine_sends.shape[1]
    group_half = group_sends.shape[1]
    fine_halo = 2 * fine_half // TILE
    group_halo = 2 * group_half // TILE
    fine_blocks = length // TILE
    group_blocks = group_length // TILE
    coarse_blocks = coarse_tiles.shape[0]

    fine_weights = fine_weights.reshape(1, -1)
    fine_groups = fine_groups.reshape(1, -1)
    group_weights = group_weights.reshape(1, -1)
    group_groups = group_groups.reshape(1, -1)
    fine_columns = fine_columns.T
    group_columns = group_columns.T
    coarse_columns = coarse_columns.T

    grp = lax.axis_index(GRP)
    mem = lax.axis_index(MEM)
    row_a = jnp.maximum((grp - 1) // 2, 0)
    row_b = jnp.minimum(row_a + 1, coarse_blocks - 1)
    place = jnp.stack(
        [grp, mem, row_a, row_b, grp * share - row_a * TILE, 1 - mem % 2, 1 - grp % 2]
    ).astype(jnp.int32)

    def block_scratch(count):
        return pltpu.VMEM((count, 2 * rhs, 2 * TILE), BF16)

    edge = shape((rhs, fine_half))
    group_edge = shape((rhs, group_half))
    field = shape((rhs, length))
    line = shape((1, length))
    small = shape((rhs, TILE))
    picked = shape((rhs, 2 * fine_half))

    pinned = [
        pltpu.with_memory_space_constraint(x, pltpu.HBM)
        for x in (fine_tiles, fine_sends, right_side, fine_weights, fine_groups, group_weights,
                  group_groups, group_sends)
    ]
    group_tiles = pltpu.with_memory_space_constraint(group_tiles, pltpu.HBM)
    coarse_tiles = pltpu.with_memory_space_constraint(coarse_tiles, pltpu.HBM)
    (fine_scale, fine_diagonal, fine_start, near, far, fine_picks, fine_tiles, right_side,
     place, fine_columns, fine_weights, fine_groups, group_weights, group_groups,
     group_sends) = run(
        functools.partial(first_kernel, lines=5), "first",
        [line, line, field, edge, edge, shape((length, 2 * fine_half), BF16),
         shape(fine_tiles.shape), field, scalars(7), pltpu.SMEM(fine_columns.shape, jnp.int32),
         line, shape((1, length), jnp.int32), line, shape((1, group_length), jnp.int32),
         shape(group_sends.shape, jnp.int32)],
        [place, fine_columns] + pinned, smem=(0, 1), hbm_args=range(2, 10), smem_outs=(8, 9),
        scratch=[pltpu.VMEM(fine_sends.shape, jnp.int32),
                 pltpu.SemaphoreType.DMA((CHUNKS + 7,))],
    )
    near, far = neighbours(near, far, ALL)
    fine_packed, fine_table, fine_visits = run(
        pack_fine_kernel, "pack_fine",
        [shape((3 * fine_blocks + 1, 2 * TILE, TILE), BF16), shape((fine_count, length), BF16),
         scalars(4 * fine_halo)],
        (fine_columns, fine_tiles, fine_groups), smem=(0,), smem_outs=(2,),
    )

    (group_scale, group_diagonal, group_tiles, group_picks, edge_near, edge_far,
     group_visits, group_columns) = run(
        group_setup_kernel, "group_setup",
        [
            line,
            line,
            shape(group_tiles.shape),
            shape((group_length, 2 * group_half), BF16),
            shape((8, group_half)),
            shape((8, group_half)),
            scalars(4 * group_halo),
            pltpu.SMEM(group_columns.shape, jnp.int32),
        ],
        (place, group_columns, group_tiles, group_sends, group_weights, group_groups),
        smem=(0, 1), smem_outs=(6, 7), hbm_args=(2,),
        scratch=[pltpu.SemaphoreType.DMA((CHUNKS,))],
    )
    facts = (edge_near, edge_far)
    def coarse_parts(after):
        return run(
            coarse_setup_kernel, "coarse_setup",
            [
                shape((coarse_blocks, 1, TILE)),
                shape((6, 2 * TILE, TILE), BF16),
                pltpu.SMEM(coarse_columns.shape, jnp.int32),
                shape((TILE, group_length), BF16),
                shape((2 * TILE, group_length), BF16),
            ],
            (place, coarse_columns, coarse_tiles, group_groups, after), smem=(0, 1),
            smem_outs=(2,), hbm_args=(2,),
            scratch=[pltpu.VMEM(coarse_tiles.shape, F32),
                     pltpu.VMEM((1, coarse_blocks * TILE), F32),
                     pltpu.SemaphoreType.DMA((CHUNKS,))],
        )

    kept = {}

    def vcycle(source, fine_start, near, far, edges, held):
        coarse = run(
            inner_restrict_kernel, "inner_restrict", [shape((rhs, fine_count))],
            (fine_columns, fine_packed, fine_diagonal, fine_start, source, fine_weights,
             fine_table),
            smem=(0,), scratch=[block_scratch(fine_blocks + fine_halo), pltpu.VMEM((rhs, length), F32)],
        )[0]
        lowered = run(
            functools.partial(restrict_kernel, spot=5, after=len(held)), "restrict",
            [shape((members, rhs, fine_count))],
            (place, fine_visits, fine_packed, coarse, far, near, fine_weights, fine_table)
            + held,
            smem=(0, 1), scratch=[block_scratch(fine_halo)],
        )[0]
        gathered = exchanged(lowered, MEM)
        extra = facts if edges is None else ()
        message = shape((rhs + 8 * bool(extra), group_half))
        group_rhs, group_start, near, far = run(
            group_start_kernel, "group_start", [field, field, message, message],
            (gathered, group_scale, group_picks) + extra,
        )
        g_near, g_far = neighbours(near, far, GRP)
        if edges is None:
            kept["coarse"] = coarse_parts(near)
            kept["packed"] = run(
                group_pack_kernel, "group_pack",
                [shape((3 * group_blocks + 1, 2 * TILE, TILE), BF16)], (group_tiles, near),
            )[0]
        group_packed = kept["packed"]
        coarse_scale, coarse_packed, coarse_cols, group_table, raise_table = kept["coarse"]
        coarse = run(
            inner_restrict_kernel, "group_inner", [shape((rhs, TILE))],
            (group_columns, group_packed, group_diagonal, group_start, group_rhs,
             group_weights, group_table),
            smem=(0,), scratch=[block_scratch(group_blocks + group_halo), pltpu.VMEM((rhs, length), F32)],
        )[0]
        payload, *made = run(
            functools.partial(group_restrict_kernel, edges=edges is None), "group_restrict",
            [shape((group_total, 16, TILE))]
            + ([shape((1, 2 * group_half)), shape((2 * TILE, 2 * group_half), BF16)]
               if edges is None else []),
            (place, group_visits, group_packed, coarse, g_far, g_near, group_weights,
             group_table) + ((coarse_scale,) if edges is None else ()),
            smem=(0, 1), scratch=[block_scratch(group_halo)],
        )
        edges = tuple(made) if edges is None else edges
        gathered = exchanged(payload, GRP)
        fine_next, near, far = run(
            coarse_kernel, "coarse", [field, edge, edge],
            (place, coarse_cols, group_columns, gathered, coarse_scale, coarse_packed,
             group_start, g_far, g_near, group_rhs, group_scale, group_diagonal, group_packed,
             group_weights, raise_table, *edges, fine_start, fine_weights, fine_table,
             fine_picks),
            smem=(0, 1, 2),
            scratch=[block_scratch(group_blocks + group_halo), pltpu.VMEM((rhs, length), F32)],
        )
        near, far = neighbours(near, far, ALL)
        inside, out = run(
            inner_smooth_kernel, "inner_smooth", [field, picked],
            (fine_columns, fine_packed, fine_diagonal, fine_next, source, fine_scale,
             fine_picks),
            smem=(0,), scratch=[block_scratch(fine_blocks + fine_halo)],
        )
        smoothed, near, far = run(
            smooth_kernel, "smooth", [field, edge, edge],
            (place, fine_visits, fine_packed, inside, out, far, near, fine_scale, fine_picks),
            smem=(0, 1), scratch=[block_scratch(fine_halo)],
        )
        near, far = neighbours(near, far, ALL)
        return smoothed, near, far, edges

    value, near, far, edges = vcycle(right_side, fine_start, near, far, None, (edge_near,))
    inside, out, sums = run(
        inner_image_kernel, "inner_image", [field, picked, small],
        (fine_columns, fine_packed, fine_diagonal, value, fine_scale, right_side, fine_picks),
        smem=(0,), scratch=[block_scratch(fine_blocks + fine_halo)],
    )
    product, start, near, far, sums = run(
        image_kernel, "image", [field, field, edge, edge, small],
        (place, fine_visits, fine_packed, inside, out, sums, far, near, fine_scale, value,
         fine_picks),
        smem=(0, 1), scratch=[block_scratch(fine_halo)],
    )
    near, far = neighbours(near, far, ALL)
    second, near, far, _ = vcycle(product, start, near, far, edges, ())
    inside, more = run(
        inner_last_kernel, "inner_last", [field, small],
        (fine_columns, fine_packed, fine_diagonal, second, right_side, value, product),
        smem=(0,), scratch=[block_scratch(fine_blocks + fine_halo)],
    )
    image, copies = run(
        last_kernel, "last", [field, shape((members, 8, TILE))],
        (place, fine_visits, fine_packed, inside, more, sums, far, near, value, second),
        smem=(0, 1), scratch=[block_scratch(fine_halo)],
    )
    copies = run(
        sum_copies_kernel, "sum_copies", [shape((group_total, 8, TILE))],
        (exchanged(copies, MEM),),
    )[0]
    parts = exchanged(copies, GRP)
    solution, residual = run(
        final_kernel, "final", [hbm((rhs, length)), hbm((rhs, length))],
        (parts, right_side, value, product, second, image),
    )
    return solution, residual


def solution(mesh):
    finer = Mesh(mesh.devices.reshape(8, 4, 4, 2), ALL)
    return jax.shard_map(
        shards,
        mesh=finer,
        in_specs=(
            P(None, ALL),
            P(ALL, None, None, None),
            P(ALL, None),
            P(ALL, None),
            P(ALL),
            P(ALL),
            P(GRP, None, None, None),
            P(GRP, None),
            P(GRP, None),
            P(GRP),
            P(GRP),
            P(),
            P(),
        ),
        out_specs=(P(None, ALL), P(None, ALL)),
        check_vma=False,
    )
```
